32 devices in a mesh: fsdp: 8 (over y, x, core), tensor: 4 (over z).
Axes of the slice: x: 2, y: 2, z: 4, core: 2. Of those that a mesh axis runs over, the one named last changes fastest.
Arguments:
- hidden: bfloat16 [16, 1536, 1280], P('fsdp', 'tensor'), may hold values from -6 to 6
- positions: int32 [16, 2, 1536], P('fsdp'), may hold values from 0 to 31
- segments: int32 [16, 1536], P('fsdp'), may hold values from 0 to 2, never falling along the last dimension, each value on 1 to 1024 neighbouring positions
- ln1_gain: bfloat16 [1280], P('fsdp'), may hold values from 0.5 to 1.5
- ln1_bias: bfloat16 [1280], P('fsdp'), may hold values from -1.25 to 1.25
- qkv_weight: bfloat16 [1280, 3, 1280], P('fsdp', None, 'tensor'), may hold values from -0.15625 to 0.15625
- qkv_bias: bfloat16 [3, 1280], P(None, 'tensor'), may hold values from -1.75 to 1.75
- proj_weight: bfloat16 [1280, 1280], P('tensor', 'fsdp'), may hold values from -2.5 to 2.5
- proj_bias: bfloat16 [1280], P('fsdp'), may hold values from -1.75 to 1.75
- ln2_gain: bfloat16 [1280], P('fsdp'), may hold values from 0.5 to 1.5
- ln2_bias: bfloat16 [1280], P('fsdp'), may hold values from -1.25 to 1.25
- fc1_weight: bfloat16 [1280, 5120], P('fsdp', 'tensor'), may hold values from -0.15625 to 0.15625
- fc1_bias: bfloat16 [5120], P('tensor'), may hold values from -1.75 to 1.75
- fc2_weight: bfloat16 [5120, 1280], P('tensor', 'fsdp'), may hold values from -0.078125 to 0.078125
- fc2_bias: bfloat16 [1280], P('fsdp'), may hold values from -1.75 to 1.75
- cotangent: bfloat16 [16, 1536, 1280], P('fsdp', 'tensor'), may hold values from -6 to 6
Outputs:
- output: bfloat16 [16, 1536, 1280], P('fsdp', 'tensor')
- hidden_grad: bfloat16 [16, 1536, 1280], P('fsdp', 'tensor')
- ln1_gain_grad: float32 [1280], P('fsdp')
- ln1_bias_grad: float32 [1280], P('fsdp')
- qkv_weight_grad: float32 [1280, 3, 1280], P('fsdp', None, 'tensor')
- qkv_bias_grad: float32 [3, 1280], P(None, 'tensor')
- proj_weight_grad: float32 [1280, 1280], P('tensor', 'fsdp')
- proj_bias_grad: float32 [1280], P('fsdp')
- ln2_gain_grad: float32 [1280], P('fsdp')
- ln2_bias_grad: float32 [1280], P('fsdp')
- fc1_weight_grad: float32 [1280, 5120], P('fsdp', 'tensor')
- fc1_bias_grad: float32 [5120], P('tensor')
- fc2_weight_grad: float32 [5120, 1280], P('tensor', 'fsdp')
- fc2_bias_grad: float32 [1280], P('fsdp')
The draws below stay inside these ranges and needn't reach their ends.
Inputs may be any that keep to these rules, and one draw needn't show every extreme that they name: `positions`: arbitrary rotary row and column indices, drawn independently for every patch. `segments`: patches of one image are contiguous in a pack and image numbers never fall; each pack holds images of 1 to 1024 patches, one of exactly 1024.
All inputs are finite; a program needn't handle non-finite values.
Results may differ from the reference program's by a relative error of at most 0.018.
Values may be sent and summed in bfloat16 or wider, within the bound.
A program may use at most 256 MiB of HBM per device.

```python
import math
import jax
import jax.numpy as jnp
import numpy as np
from jax import lax

D = 1280
FF = 5120
HEADS = 16
HEAD_DIM = 80
PACK = 1536
IMAGE_MOST = 1024
GRID = 32
IMGS_PACK = 3
PACKS = 16


def place_ends(drawn, key, low, top_value):
    extent = drawn.shape
    index_at = [jax.random.randint(jax.random.fold_in(key, axis), (), 0, extent[axis]) for axis in range(len(extent))]
    drawn = drawn.at[tuple(index_at)].set(low)
    longest = extent.index(max(extent))
    index_at[longest] = (index_at[longest] + 1) % extent[longest]
    return drawn.at[tuple(index_at)].set(top_value)


def strengthened(entries, stream_key, source, target, parts, factor):
    owner, partner = [(jnp.arange(entries.shape[position]) // (entries.shape[position] // parts)).reshape([-1 if axis == position else 1 for axis in range(entries.ndim)]) for position in (source, target)]
    chosen = jax.random.permutation(stream_key, parts)[partner]
    strong = (owner == chosen) | (owner == (partner + parts // 2) % parts)
    return jnp.where(strong, factor * entries, entries)


def levels(rng, dims, cuts, low, top_value):
    factor_of, own = 1.0, jax.random.fold_in(rng, 6)
    for dim, parts in cuts:
        steps = jnp.exp(jax.random.uniform(jax.random.fold_in(own, dim), (parts,), jnp.float32, low / len(cuts), top_value / len(cuts)))
        factor_of = factor_of * jnp.repeat(steps, dims[dim] // parts).reshape([-1 if axis == dim else 1 for axis in range(len(dims))])
    return factor_of


def length_profile(amount, total, bound, lean):
    loads = [(1 << 20) // math.isqrt(rank ** lean) + 1 for rank in range(2, amount + 1)]
    rest, given = total - bound - (amount - 1), [1] * (amount - 1)
    while rest > 0:
        movable = [i for i in range(amount - 1) if given[i] < bound]
        whole, budget = sum([loads[i] for i in movable]), rest
        for i in movable:
            more = min(bound - given[i], max(1, budget * loads[i] // whole), rest)
            given[i] = given[i] + more
            rest = rest - more
    return np.array([bound] + given)


def ragged_sizes(own_key, count, total, limit, lean):
    if count == 2:
        one = jax.random.randint(own_key, (), max(1, total - limit), min(limit, total - 1) + 1)
        return jnp.stack([one, total - one])
    sizes = jnp.asarray(length_profile(count, total, limit, lean), jnp.int32)
    twos = (count - 1) // 2
    donor, sink = sizes[1:1 + 2 * twos:2], sizes[2:2 + 2 * twos:2]
    slack = jnp.minimum(donor - 1, limit - sink)
    shifted = jax.random.randint(jax.random.fold_in(own_key, 1), (twos,), 0, 1 << 20) % (slack + 1)
    sizes = sizes.at[1:1 + 2 * twos:2].set(donor - shifted).at[2:2 + 2 * twos:2].set(sink + shifted)
    return sizes[jax.random.permutation(jax.random.fold_in(own_key, 2), count)]


def normal_values(rng, shape, scale, limit, shards=(), kind=jnp.bfloat16):
    drawn = scale * jax.random.normal(rng, shape, jnp.float32)
    if shards:
        drawn = drawn * levels(rng, shape, shards, -0.22, 0.18)
    return jnp.clip(drawn, -limit, limit).astype(kind)


def gaussian_with(key, shape, width, most, split, heavy, held_as=jnp.bfloat16):
    entries = width * jax.random.normal(key, shape, jnp.float32)
    if split:
        entries = entries * levels(key, shape, split, -0.22, 0.18)
    return jnp.clip(strengthened(entries, jax.random.fold_in(key, 3), *heavy), -most, most).astype(held_as)


def setup_inputs(seed: int = 0) -> dict:
    streams_of = jax.random.split(jax.random.key(seed), 17)
    return {
        "hidden": gaussian_with(streams_of[0], (PACKS, PACK, D), 1.0, 6.0, ((0, 8), (1, 4)), (0, 2, 8, 2.0)),
        "positions": place_ends(jax.random.randint(streams_of[1], (PACKS, 2, PACK), 0, GRID), jax.random.fold_in(streams_of[1], 1), 0, GRID - 1).astype(jnp.int32),
        "segments": jax.vmap(lambda own: jnp.searchsorted(jnp.cumsum(ragged_sizes(own, IMGS_PACK, PACK, IMAGE_MOST, 0)), jnp.arange(PACK), side="right"))(jax.random.split(streams_of[2], PACKS)).reshape((PACKS, PACK)).astype(jnp.int32),
        "ln1_gain": jnp.clip(1.0 + 0.1 * jax.random.normal(streams_of[3], (D,), jnp.float32), 0.5, 1.5).astype(jnp.bfloat16),
        "ln1_bias": normal_values(streams_of[4], (D,), 0.2, 1.25, ((0, 8),)),
        "qkv_weight": normal_values(streams_of[5], (D, 3, D), D ** -0.5, 0.15625, ((0, 8), (2, 4))),
        "qkv_bias": normal_values(streams_of[6], (3, D), 0.3, 1.75, ((1, 4),)),
        "proj_weight": normal_values(streams_of[7], (D, D), (max(1, D // 256)) ** -0.5, 2.5, ((0, 4), (1, 8))),
        "proj_bias": normal_values(streams_of[8], (D,), 0.3, 1.75, ((0, 8),)),
        "ln2_gain": jnp.clip(1.0 + 0.1 * jax.random.normal(streams_of[9], (D,), jnp.float32), 0.5, 1.5).astype(jnp.bfloat16),
        "ln2_bias": normal_values(streams_of[10], (D,), 0.2, 1.25, ((0, 8),)),
        "fc1_weight": normal_values(streams_of[11], (D, FF), D ** -0.5, 0.15625, ((0, 8), (1, 4))),
        "fc1_bias": normal_values(streams_of[12], (FF,), 0.3, 1.75, ((0, 4),)),
        "fc2_weight": normal_values(streams_of[13], (FF, D), FF ** -0.5, 0.078125, ((0, 4), (1, 8))),
        "fc2_bias": normal_values(streams_of[14], (D,), 0.3, 1.75, ((0, 8),)),
        "cotangent": gaussian_with(streams_of[15], (PACKS, PACK, D), 1.0, 6.0, ((0, 8), (1, 4)), (0, 2, 8, 2.0)),
    }


epsilon = 1e-06

@jax.custom_vjp
def low(v):
    return lax.optimization_barrier(v.astype(jnp.bfloat16)).astype(jnp.float32)

@jax.custom_vjp
def low_back(v):
    return v

def low_keep(v):
    return (low(v), None)

def low_pass(kept, grad):
    return (grad,)

def back_keep(v):
    return (v, None)

def back_low(kept, grad):
    return (low(grad),)
low.defvjp(low_keep, low_pass)
low_back.defvjp(back_keep, back_low)

def angle_tables(place):
    quarter = HEAD_DIM // 4
    freqs = 10000.0 ** (-(4.0 * jnp.arange(quarter, dtype=jnp.float32)) / HEAD_DIM)
    row_angles = place[0].astype(jnp.float32)[:, None] * freqs[None, :]
    col_angles = place[1].astype(jnp.float32)[:, None] * freqs[None, :]
    halfway = jnp.concatenate([row_angles, col_angles], axis=1)
    angles = jnp.concatenate([halfway, halfway], axis=1)
    return (jnp.cos(angles), jnp.sin(angles))

def rotate(values, cosine, sine):
    middle_index = HEAD_DIM // 2
    turned = jnp.concatenate([-values[..., middle_index:], values[..., :middle_index]], axis=-1)
    return values * cosine[:, None, :] + turned * sine[:, None, :]

def normalize(values, gain, shift):
    center = values - lax.optimization_barrier(jnp.mean(values, axis=-1, keepdims=True))
    spread = lax.rsqrt(lax.optimization_barrier(jnp.mean(center * center, axis=-1, keepdims=True)) + epsilon)
    return center * spread * gain + shift

def attention(queries, keys, values, labels):
    total = queries.shape[0]
    block = min(512, total)
    count = total // block
    scale = HEAD_DIM ** (-0.5)
    highest = lax.Precision.HIGHEST

    def one_block(pair):
        query_block, label_block = pair
        scores = low_back(jnp.einsum('qhd,khd->hqk', query_block, keys, precision=highest) * scale)
        same_image = label_block[:, None] == labels[None, :]
        scores = jnp.where(same_image[None, :, :], scores, -1000000000.0)
        log_total = jax.nn.logsumexp(scores, axis=-1, keepdims=True)
        weights = low(jnp.exp(scores - log_total))
        return jnp.einsum('hqk,khd->qhd', weights, values, precision=highest)
    mixed = lax.map(jax.checkpoint(one_block), (queries.reshape(count, block, HEADS, HEAD_DIM), labels.reshape(count, block)))
    return mixed.reshape(total, HEADS * HEAD_DIM)

def layer(hidden, ln1_gain, ln1_bias, qkv_weight, qkv_bias, proj_weight, proj_bias, ln2_gain, ln2_bias, fc1_weight, fc1_bias, fc2_weight, fc2_bias, cosine, sine, labels):
    highest = lax.Precision.HIGHEST
    total = hidden.shape[0]
    normed = low(normalize(hidden, ln1_gain, ln1_bias))
    projected = low_back(jnp.einsum('pd,dtc->ptc', normed, qkv_weight, precision=highest) + qkv_bias)
    queries = low(rotate(projected[:, 0].reshape(total, HEADS, HEAD_DIM), cosine, sine))
    keys = low(rotate(projected[:, 1].reshape(total, HEADS, HEAD_DIM), cosine, sine))
    values = low(projected[:, 2].reshape(total, HEADS, HEAD_DIM))
    mixed = low_back(low(attention(queries, keys, values, labels)))
    branch = low_back(jnp.dot(mixed, proj_weight, precision=highest))
    middle = hidden + branch + proj_bias
    normed_two = low(normalize(middle, ln2_gain, ln2_bias))
    before = low_back(jnp.dot(normed_two, fc1_weight, precision=highest) + fc1_bias)
    after = low(before * jax.nn.sigmoid(1.702 * before))
    return middle + low_back(jnp.dot(after, fc2_weight, precision=highest)) + fc2_bias

def reference(hidden, positions, segments, ln1_gain, ln1_bias, qkv_weight, qkv_bias, proj_weight, proj_bias, ln2_gain, ln2_bias, fc1_weight, fc1_bias, fc2_weight, fc2_bias, cotangent):
    params = tuple((weight.astype(jnp.float32) for weight in (ln1_gain, ln1_bias, qkv_weight, qkv_bias, proj_weight, proj_bias, ln2_gain, ln2_bias, fc1_weight, fc1_bias, fc2_weight, fc2_bias)))

    def per_pack(sums, inputs):
        pack_hidden, place, labels, pack_grad = inputs
        cosine, sine = angle_tables(place)

        def forward(pack_input, *weights):
            return layer(pack_input, *weights, cosine, sine, labels)
        result, pullback = jax.vjp(forward, pack_hidden.astype(jnp.float32), *params)
        grads = pullback(pack_grad.astype(jnp.float32))
        sums = tuple((running + update for running, update in zip(sums, grads[1:])))
        return (sums, (result.astype(jnp.bfloat16), grads[0].astype(jnp.bfloat16)))
    zeros = tuple((jnp.zeros_like(weight) for weight in params))
    sums, (output, hidden_grad) = lax.scan(per_pack, zeros, (hidden, positions, segments, cotangent))
    return (output, hidden_grad, sums[0], sums[1], sums[2], sums[3], sums[4], sums[5], sums[6], sums[7], sums[8], sums[9], sums[10], sums[11])
```

```python
import jax
import jax.numpy as jnp
from jax import lax
from jax.sharding import Mesh, PartitionSpec as P

HEAD_DIM = 80

epsilon = 1e-06


def angle_tables(place):
    quarter = HEAD_DIM // 4
    freqs = 10000.0 ** (-(4.0 * jnp.arange(quarter, dtype=jnp.float32)) / HEAD_DIM)
    row_angles = place[0].astype(jnp.float32)[:, None] * freqs[None, :]
    col_angles = place[1].astype(jnp.float32)[:, None] * freqs[None, :]
    halfway = jnp.concatenate([row_angles, col_angles], axis=1)
    angles = jnp.concatenate([halfway, halfway], axis=1)
    return (jnp.cos(angles), jnp.sin(angles))


def rotate(values, cosine, sine):
    middle_index = HEAD_DIM // 2
    turned = jnp.concatenate([-values[..., middle_index:], values[..., :middle_index]], axis=-1)
    return values * cosine[:, None, :] + turned * sine[:, None, :]


def rotate_back(grads, cosine, sine):
    middle_index = HEAD_DIM // 2
    scaled = grads * sine[:, None, :]
    turned = jnp.concatenate([scaled[..., middle_index:], -scaled[..., :middle_index]], axis=-1)
    return grads * cosine[:, None, :] + turned


def normalize(values, gain, shift):
    center = values - jnp.mean(values, axis=-1, keepdims=True)
    spread = lax.rsqrt(jnp.mean(center * center, axis=-1, keepdims=True) + epsilon)
    unit = center * spread
    return (unit * gain + shift, unit, spread)


def normalize_back(grads, unit, spread, gain):
    scaled = grads * gain
    inner = (
        scaled
        - jnp.mean(scaled, axis=-1, keepdims=True)
        - unit * jnp.mean(scaled * unit, axis=-1, keepdims=True)
    )
    return inner * spread


def masked_scores(query_block, label_block, keys, labels, scale):
    scores = (
        jnp.einsum("qhd,khd->hqk", query_block, keys, preferred_element_type=jnp.float32) * scale
    )
    same_image = label_block[:, None] == labels[None, :]
    return jnp.where(same_image[None, :, :], scores, -1000000000.0)


def attend(queries, keys, values, labels):
    total, heads, width = queries.shape
    block = min(512, total)
    count = total // block
    scale = width ** (-0.5)

    def one_block(pair):
        query_block, label_block = pair
        scores = masked_scores(query_block, label_block, keys, labels, scale)
        largest = jnp.max(scores, axis=-1, keepdims=True)
        log_total = largest + jnp.log(jnp.sum(jnp.exp(scores - largest), axis=-1, keepdims=True))
        weights = jnp.exp(scores - log_total).astype(jnp.bfloat16)
        mixed = jnp.einsum("hqk,khd->qhd", weights, values, preferred_element_type=jnp.float32)
        return (mixed.astype(jnp.bfloat16), log_total[..., 0])

    mixed, log_total = lax.map(
        one_block, (queries.reshape(count, block, heads, width), labels.reshape(count, block))
    )
    return (mixed.reshape(total, heads * width), log_total)


def attend_back(queries, keys, values, labels, mixed_grad, log_total):
    total, heads, width = queries.shape
    block = min(512, total)
    count = total // block
    scale = width ** (-0.5)

    def one_block(carry, inputs):
        key_grad, value_grad = carry
        query_block, label_block, out_grad, block_total = inputs
        scores = masked_scores(query_block, label_block, keys, labels, scale)
        probs = jnp.exp(scores - block_total[:, :, None])
        rounded = probs.astype(jnp.bfloat16)
        value_grad = value_grad + jnp.einsum(
            "hqk,qhd->khd", rounded, out_grad, preferred_element_type=jnp.float32
        )
        weight_grad = jnp.einsum(
            "qhd,khd->hqk", out_grad, values, preferred_element_type=jnp.float32
        )
        row_inner = jnp.sum(probs * weight_grad, axis=-1, keepdims=True)
        score_grad = (probs * (weight_grad - row_inner)).astype(jnp.bfloat16)
        query_grad = (
            jnp.einsum("hqk,khd->qhd", score_grad, keys, preferred_element_type=jnp.float32) * scale
        )
        key_grad = (
            key_grad
            + jnp.einsum(
                "hqk,qhd->khd", score_grad, query_block, preferred_element_type=jnp.float32
            )
            * scale
        )
        return ((key_grad, value_grad), query_grad)

    zeros = jnp.zeros((total, heads, width), jnp.float32)
    (key_grad, value_grad), query_grad = lax.scan(
        one_block,
        (zeros, zeros),
        (
            queries.reshape(count, block, heads, width),
            labels.reshape(count, block),
            mixed_grad.reshape(count, block, heads, width),
            log_total,
        ),
    )
    return (query_grad.reshape(total, heads, width), key_grad, value_grad)


def swap(values):
    return lax.ppermute(values, "c", [(0, 1), (1, 0)])


def travel(step, size):
    runs = size // 2
    pairs = []
    for core in range(2):
        for place in range(size):
            half, part = divmod(place, runs)
            pairs.append((core * size + place, half * size + runs * core + (part + step) % runs))
    return pairs


def bring(packs, place, size):
    runs = size // 2
    parts = [
        lax.ppermute(
            lax.dynamic_index_in_dim(packs, lax.rem(place + step, runs), 0, keepdims=False),
            ("c", "z"),
            travel(step, size),
        )
        for step in range(runs)
    ]
    return jnp.concatenate(parts, axis=0)


def take_back(rows, place, size):
    runs = size // 2
    count = rows.shape[0] // runs
    parts = jnp.stack(
        [
            lax.ppermute(
                rows[step * count : (step + 1) * count],
                ("c", "z"),
                [(target, source) for source, target in travel(step, size)],
            )
            for step in range(runs)
        ]
    )
    return jnp.stack(
        [
            lax.dynamic_index_in_dim(
                parts, lax.rem(index + size - place, runs), 0, keepdims=False
            )
            for index in range(runs)
        ]
    )


def pair_sum(partial):
    count = partial.shape[0] // 2
    return partial[:count] + swap(partial[count:].astype(jnp.bfloat16)).astype(jnp.float32)


def share(own):
    return jnp.concatenate([own, swap(own)], axis=0)


def gather_all(block):
    return lax.all_gather(block, ("z", "g"), axis=0, tiled=True)


def scatter_all(total):
    depth, cols = total.shape[-2:]
    return lax.psum_scatter(
        total.reshape(-1, cols), ("z", "g"), scatter_dimension=0, tiled=True
    )


def dot(form, left, right):
    return jnp.einsum(form, left, right, preferred_element_type=jnp.float32)


def on_device(
    hidden,
    positions,
    segments,
    ln1_gain,
    ln1_bias,
    qkv_weight,
    qkv_bias,
    proj_weight,
    proj_bias,
    ln2_gain,
    ln2_bias,
    fc1_weight,
    fc1_bias,
    fc2_weight,
    fc2_bias,
    cotangent,
):
    wide = jnp.float32
    size = lax.axis_size("z")
    core = lax.axis_index("c")
    place = lax.axis_index("z")
    group = lax.axis_index("g")
    batches, rows, width = hidden.shape
    runs = size // 2
    assert batches == runs
    shard = qkv_weight.shape[0]
    local_cols = qkv_weight.shape[2]
    half_cols = local_cols // 2
    units = fc1_weight.shape[1]
    half_units = units // 2
    heads = size * half_cols // HEAD_DIM
    total = 2 * runs * rows
    first = core == 0

    first_part = jnp.concatenate(
        [
            qkv_weight.reshape(shard, 3, 2, half_cols).transpose(0, 2, 1, 3).reshape(
                shard, 2, 3 * half_cols
            ),
            proj_weight.T.reshape(shard, 2, half_cols),
        ],
        axis=2,
    )
    packed = jnp.concatenate(
        [
            first_part,
            fc1_weight.reshape(shard, 2, half_units),
            fc2_weight.T.reshape(shard, 2, half_units),
        ],
        axis=2,
    )
    keep = jnp.where(first, packed[:, 0], packed[:, 1])
    other = swap(jnp.where(first, packed[:, 1], packed[:, 0]))
    block = jnp.where(
        first, jnp.concatenate([keep, other], axis=0), jnp.concatenate([other, keep], axis=0)
    )
    attn_cols = 4 * half_cols
    attn_full = gather_all(block[:, :attn_cols]).reshape(size, width, attn_cols)
    fc1_full = gather_all(block[:, attn_cols : attn_cols + half_units]).reshape(
        size, width, half_units
    )
    fc2_full = gather_all(block[:, attn_cols + half_units :]).reshape(size, width, half_units)
    qkv_full = attn_full[:, :, : 3 * half_cols].reshape(size, width, 3, half_cols)
    proj_full = attn_full[:, :, 3 * half_cols :]

    small = jnp.concatenate(
        [
            ln1_gain,
            ln1_bias,
            proj_bias,
            ln2_gain,
            ln2_bias,
            fc2_bias,
            qkv_bias.reshape(-1),
            fc1_bias,
        ]
    )
    small_full = lax.all_gather(small, ("g", "c", "z"), axis=0).reshape(-1, size, small.shape[0])
    vectors = (
        small_full[:, 0, : 6 * shard].reshape(-1, 6, shard).transpose(1, 0, 2).reshape(6, width)
    ).astype(wide)
    gain_one, shift_one, proj_shift, gain_two, shift_two, fc2_shift = (
        vectors[index] for index in range(6)
    )
    tail = small_full[0, :, 6 * shard :].astype(wide)
    qkv_shifts = tail[:, : 3 * local_cols].reshape(size, 3, 2, half_cols)
    qkv_shift = jnp.where(first, qkv_shifts[:, :, 0], qkv_shifts[:, :, 1]).transpose(1, 0, 2)
    fc1_shifts = tail[:, 3 * local_cols :].reshape(size, 2, half_units)
    fc1_shift = jnp.where(first, fc1_shifts[:, 0], fc1_shifts[:, 1])

    marks = jnp.concatenate([positions, segments[:, None, :]], axis=1)
    marks_other = swap(marks)
    own_pack = place // runs == core
    batch = lax.rem(place, runs)
    marks = lax.dynamic_index_in_dim(
        jnp.where(own_pack, marks, marks_other), batch, 0, keepdims=False
    ).reshape(3, size, rows)
    order = [
        runs * (core if side == 0 else 1 - core) + lax.rem(batch + runs - step, runs)
        for side in range(2)
        for step in range(runs)
    ]
    marks = jnp.concatenate(
        [lax.dynamic_index_in_dim(marks, index, 1, keepdims=False) for index in order], axis=1
    )
    cosine, sine = angle_tables(marks[:2])
    labels = marks[2]

    start_values = bring(hidden, place, size).astype(wide)
    out_grad = bring(cotangent, place, size)
    normed, unit_one, spread_one = normalize(start_values, gain_one, shift_one)
    normed_full = share(normed.astype(jnp.bfloat16))
    projected = dot("pd,zdtc->ptzc", normed_full, qkv_full) + qkv_shift
    split = projected.reshape(total, 3, heads, HEAD_DIM)
    queries = rotate(split[:, 0], cosine, sine).astype(jnp.bfloat16)
    keys = rotate(split[:, 1], cosine, sine).astype(jnp.bfloat16)
    values = split[:, 2].astype(jnp.bfloat16)
    mixed, log_total = attend(queries, keys, values, labels)
    mixed = mixed.reshape(total, size, half_cols)
    middle = start_values + pair_sum(dot("pzk,zdk->pd", mixed, proj_full)) + proj_shift
    normed_two, unit_two, spread_two = normalize(middle, gain_two, shift_two)
    ffn_input = share(normed_two.astype(jnp.bfloat16))
    before = dot("pd,zdf->pzf", ffn_input, fc1_full) + fc1_shift
    sigma = jax.nn.sigmoid(1.702 * before)
    after = (before * sigma).astype(jnp.bfloat16)
    outcome = middle + pair_sum(dot("pzf,zdf->pd", after, fc2_full)) + fc2_shift
    output = take_back(outcome.astype(jnp.bfloat16), place, size)

    out_grad_wide = out_grad.astype(wide)
    out_grad_full = share(out_grad)
    fc2_part = scatter_all(dot("pd,pzf->zdf", out_grad_full, after).astype(jnp.bfloat16))
    after_grad = dot("pd,zdf->pzf", out_grad_full, fc2_full)
    before_grad = (after_grad * (sigma + 1.702 * before * sigma * (1.0 - sigma))).astype(
        jnp.bfloat16
    )
    fc1_part = scatter_all(dot("pd,pzf->zdf", ffn_input, before_grad).astype(jnp.bfloat16))
    fc1_bias_total = jnp.sum(before_grad.astype(wide), axis=0)
    normed_two_grad = pair_sum(dot("pzf,zdf->pd", before_grad, fc1_full))
    middle_grad = out_grad_wide + normalize_back(normed_two_grad, unit_two, spread_two, gain_two)
    branch_grad_full = share(middle_grad.astype(jnp.bfloat16))
    proj_grad = dot("pd,pzk->zdk", branch_grad_full, mixed).astype(jnp.bfloat16)
    mixed_grad = dot("pd,zdk->pzk", branch_grad_full, proj_full).astype(jnp.bfloat16)
    query_turned, key_turned, value_grad = attend_back(
        queries, keys, values, labels, mixed_grad.reshape(total, heads, HEAD_DIM), log_total
    )
    projected_grad = jnp.stack(
        [
            rotate_back(query_turned, cosine, sine).reshape(total, size, half_cols),
            rotate_back(key_turned, cosine, sine).reshape(total, size, half_cols),
            value_grad.reshape(total, size, half_cols),
        ],
        axis=2,
    ).astype(jnp.bfloat16)
    qkv_bias_total = jnp.sum(projected_grad.astype(wide), axis=0)
    qkv_grad = dot("pd,pztc->zdtc", normed_full, projected_grad).astype(jnp.bfloat16)
    attn_part = scatter_all(
        jnp.concatenate([qkv_grad.reshape(size, width, 3 * half_cols), proj_grad], axis=2)
    )
    normed_grad = pair_sum(dot("pztc,zdtc->pd", projected_grad, qkv_full))
    hidden_grad = middle_grad + normalize_back(normed_grad, unit_one, spread_one, gain_one)
    input_grad = take_back(hidden_grad.astype(jnp.bfloat16), place, size)

    def halves(values):
        zero = jnp.zeros_like(values)
        return jnp.where(first, jnp.stack([values, zero], 1), jnp.stack([zero, values], 1))

    small_sums = lax.psum(
        jnp.concatenate(
            [
                jnp.concatenate(
                    [
                        jnp.sum(normed_grad * unit_one, axis=0),
                        jnp.sum(normed_grad, axis=0),
                        jnp.sum(middle_grad, axis=0),
                        jnp.sum(normed_two_grad * unit_two, axis=0),
                        jnp.sum(normed_two_grad, axis=0),
                        jnp.sum(out_grad_wide, axis=0),
                    ]
                ),
                halves(qkv_bias_total.reshape(size, 3 * half_cols)).reshape(-1),
                halves(fc1_bias_total).reshape(-1),
            ]
        ),
        ("g", "c", "z"),
    )
    start = 6 * width
    vector_sums = lax.dynamic_slice_in_dim(
        small_sums[:start].reshape(6, width), (2 * group + core) * shard, shard, 1
    )
    middle_at = start + size * 3 * local_cols
    qkv_bias_sum = lax.dynamic_index_in_dim(
        small_sums[start:middle_at].reshape(size, 2, 3, half_cols), place, 0, keepdims=False
    )
    qkv_bias_sum = qkv_bias_sum.transpose(1, 0, 2).reshape(3, local_cols)
    fc1_bias_sum = lax.dynamic_index_in_dim(
        small_sums[middle_at:].reshape(size, units), place, 0, keepdims=False
    )

    def own_rows(part):
        mine = jnp.where(first, part[:shard], part[shard:])
        theirs = swap(jnp.where(first, part[shard:], part[:shard]))
        return jnp.where(first, jnp.stack([mine, theirs]), jnp.stack([theirs, mine])).astype(wide)

    fc2_sum = own_rows(fc2_part).transpose(0, 2, 1).reshape(units, shard)
    fc1_sum = own_rows(fc1_part).transpose(1, 0, 2).reshape(shard, units)
    attn_sum = own_rows(attn_part)
    qkv_sum = (
        attn_sum[:, :, : 3 * half_cols]
        .reshape(2, shard, 3, half_cols)
        .transpose(1, 2, 0, 3)
        .reshape(shard, 3, local_cols)
    )
    proj_sum = attn_sum[:, :, 3 * half_cols :].transpose(0, 2, 1).reshape(local_cols, shard)
    return (
        output,
        input_grad,
        vector_sums[0],
        vector_sums[1],
        qkv_sum,
        qkv_bias_sum,
        proj_sum,
        vector_sums[2],
        vector_sums[3],
        vector_sums[4],
        fc1_sum,
        fc1_bias_sum,
        fc2_sum,
        vector_sums[5],
    )


def solution(mesh):
    fsdp, tensor = mesh.shape["fsdp"], mesh.shape["tensor"]
    cut = Mesh(mesh.devices.reshape(fsdp // 2, 2, tensor), ("g", "c", "z"))
    f = ("g", "c")
    in_specs = (
        P(f, "z", None),
        P(f, None, None),
        P(f, None),
        P(f),
        P(f),
        P(f, None, "z"),
        P(None, "z"),
        P("z", f),
        P(f),
        P(f),
        P(f),
        P(f, "z"),
        P("z"),
        P("z", f),
        P(f),
        P(f, "z", None),
    )
    out_specs = (
        P(f, "z", None),
        P(f, "z", None),
        P(f),
        P(f),
        P(f, None, "z"),
        P(None, "z"),
        P("z", f),
        P(f),
        P(f),
        P(f),
        P(f, "z"),
        P("z"),
        P("z", f),
        P(f),
    )
    return jax.shard_map(
        on_device, mesh=cut, in_specs=in_specs, out_specs=out_specs, check_vma=False
    )
```

```python
import jax
import jax.numpy as jnp
import numpy as np
from jax import lax
from jax.experimental import pallas as pl
from jax.experimental.pallas import tpu as pltpu
from jax.sharding import Mesh, PartitionSpec as P

HEAD_DIM = 80

epsilon = 1e-06


LANES = 128
HALF = LANES // 2
MID = HEAD_DIM // 2
FREE = HALF - MID
FAR = -1.0e9
LOG2E = 1.4426950408889634
SCALE = HEAD_DIM ** (-0.5)
BLOCK = 256


def angle_tables(place):
    quarter = HEAD_DIM // 4
    freqs = 10000.0 ** (-(4.0 * jnp.arange(quarter, dtype=jnp.float32)) / HEAD_DIM)
    row_angles = place[0].astype(jnp.float32)[:, None] * freqs[None, :]
    col_angles = place[1].astype(jnp.float32)[:, None] * freqs[None, :]
    half = jnp.concatenate([row_angles, col_angles], axis=1)
    cosine = jnp.pad(jnp.cos(half), ((0, 0), (0, FREE)))
    sine = jnp.pad(jnp.sin(half), ((0, 0), (0, FREE)))
    return (
        jnp.concatenate([cosine, cosine], axis=1),
        jnp.concatenate([-sine, sine], axis=1),
    )


def label_tables(labels):
    lane = jnp.arange(LANES)[None, :] - MID
    free = (lane >= 0) & (lane < FREE)
    same = lane == labels[:, None]
    return (
        jnp.where(free & same, 1.0, 0.0).astype(jnp.bfloat16),
        jnp.where(free & ~same, FAR, 0.0).astype(jnp.bfloat16),
    )


def lane_of(index):
    return index if index < MID else index - MID + HALF


def pad_tables(cols):
    heads = cols // HEAD_DIM
    first = np.zeros((4 * cols, heads * 3 * LANES), np.float32)
    second = np.zeros((4 * cols, heads * LANES), np.float32)
    for head in range(heads):
        for index in range(HEAD_DIM):
            for kind in range(3):
                source = kind * cols + head * HEAD_DIM + index
                first[source, (head * 3 + kind) * LANES + lane_of(index)] = 1.0
            source = 3 * cols + head * HEAD_DIM + index
            second[source, head * LANES + lane_of(index)] = 1.0
    return jnp.asarray(first, jnp.bfloat16), jnp.asarray(second, jnp.bfloat16)


def product(left, right, dims):
    return lax.dot_general(left, right, (dims, ((), ())), preferred_element_type=jnp.float32)


def attend_kernel(
    x_ref, w_ref, b_ref, cos_ref, sin_ref, qa_ref, ka_ref, qkv_ref, o_ref, total_ref, vt_ref
):
    total = x_ref.shape[0]
    weight = w_ref[0]
    shift = b_ref[0]
    ones = jnp.where(lax.broadcasted_iota(jnp.int32, (BLOCK, LANES), 1) == LANES - 1, 1.0, 0.0)

    def project(index, carry):
        at = pl.ds(pl.multiple_of(index * BLOCK, BLOCK), BLOCK)
        made = product(x_ref[at, :], weight, ((1,), (0,))) + shift
        cosine, sine = cos_ref[at, :], sin_ref[at, :]
        query, key = made[:, :LANES], made[:, LANES : 2 * LANES]
        value = made[:, 2 * LANES :] + ones
        query = query * cosine + pltpu.roll(query, HALF, 1) * sine
        key = key * cosine + pltpu.roll(key, HALF, 1) * sine
        qkv_ref[at, :LANES] = (query * (SCALE * LOG2E)).astype(jnp.bfloat16) + qa_ref[at, :]
        qkv_ref[at, LANES : 2 * LANES] = key.astype(jnp.bfloat16) + ka_ref[at, :]
        qkv_ref[at, 2 * LANES :] = value.astype(jnp.bfloat16)
        vt_ref[:, at] = value.T.astype(jnp.bfloat16)
        return carry

    lax.fori_loop(0, total // BLOCK, project, 0)

    def mix(index, carry):
        at = pl.ds(pl.multiple_of(index * BLOCK, BLOCK), BLOCK)
        scores = product(qkv_ref[:, LANES : 2 * LANES], qkv_ref[at, :LANES], ((1,), (1,)))
        largest = jnp.max(scores, axis=0, keepdims=True)
        probs = jnp.exp2(scores - largest).astype(jnp.bfloat16)
        mixed = product(vt_ref[...], probs, ((1,), (0,)))
        amount = mixed[LANES - 1 :, :]
        o_ref[at, :] = (mixed * (1.0 / amount)).T.astype(jnp.bfloat16)
        total_ref[0, :, at] = largest + jnp.log2(amount)
        return carry

    lax.fori_loop(0, total // BLOCK, mix, 0)


def attend(normed, weight, shift, cosine, sine, query_mark, key_mark):
    total, width = normed.shape
    size = weight.shape[0]
    pairs = weight.shape[2] // (3 * LANES)
    heads = size * pairs
    whole = lambda cols: pl.BlockSpec((total, cols), lambda h: (0, 0), pipeline_mode=pl.Buffered(1))
    return pl.pallas_call(
        attend_kernel,
        grid=(heads,),
        in_specs=[
            whole(width),
            pl.BlockSpec((1, width, 3 * LANES), lambda h: (h // pairs, 0, h % pairs)),
            pl.BlockSpec((1, 1, 3 * LANES), lambda h: (h, 0, 0)),
            whole(LANES),
            whole(LANES),
            whole(LANES),
            whole(LANES),
        ],
        out_specs=[
            pl.BlockSpec((total, 3 * LANES), lambda h: (0, h)),
            pl.BlockSpec((total, LANES), lambda h: (0, h)),
            pl.BlockSpec((1, 1, total), lambda h: (h, 0, 0)),
        ],
        out_shape=[
            jax.ShapeDtypeStruct((total, heads * 3 * LANES), jnp.bfloat16),
            jax.ShapeDtypeStruct((total, heads * LANES), jnp.bfloat16),
            jax.ShapeDtypeStruct((heads, 1, total), jnp.float32),
        ],
        scratch_shapes=[pltpu.VMEM((LANES, total), jnp.bfloat16)],
        compiler_params=pltpu.CompilerParams(vmem_limit_bytes=40 * 2**20),
        cost_estimate=pl.CostEstimate(
            flops=2 * heads * total * LANES * (3 * width + 4 * total),
            bytes_accessed=8 * total * heads * LANES + 2 * total * width,
            transcendentals=heads * total * total,
        ),
    )(normed, weight, shift, cosine, sine, query_mark, key_mark)


def back_kernel(
    qkv_ref, o_ref, grad_ref, total_ref, cos_ref, sin_ref, out_ref, bias_ref, kt_ref, dk_ref, dv_ref
):
    total = qkv_ref.shape[0]
    dk_ref[...] = jnp.zeros_like(dk_ref)
    dv_ref[...] = jnp.zeros_like(dv_ref)
    kt_ref[...] = qkv_ref[:, LANES : 2 * LANES].T

    def turn_back(grads, at):
        return (grads * cos_ref[at, :] + pltpu.roll(grads * sin_ref[at, :], HALF, 1)).astype(
            jnp.bfloat16
        )

    def step(index, carry):
        at = pl.ds(pl.multiple_of(index * BLOCK, BLOCK), BLOCK)
        query = qkv_ref[at, :LANES]
        grad = grad_ref[at, :]
        inner = grad.astype(jnp.float32) * o_ref[at, :].astype(jnp.float32)
        row = jnp.sum(inner.T, axis=0, keepdims=True)
        scores = product(qkv_ref[:, LANES : 2 * LANES], query, ((1,), (1,)))
        probs = jnp.exp2(scores - total_ref[0, :, at])
        weight_grad = product(qkv_ref[:, 2 * LANES :], grad, ((1,), (1,)))
        score_grad = (probs * (weight_grad - row)).astype(jnp.bfloat16)
        dv_ref[...] += product(probs.astype(jnp.bfloat16), grad, ((1,), (0,)))
        dk_ref[...] += product(score_grad, query, ((1,), (0,)))
        turned = product(kt_ref[...], score_grad, ((1,), (0,))).T * SCALE
        made = turn_back(turned, at)
        out_ref[at, :LANES] = made
        return carry + jnp.sum(made.astype(jnp.float32), axis=0, keepdims=True)

    zero = jnp.zeros((1, LANES), jnp.float32)
    query_bias = lax.fori_loop(0, total // BLOCK, step, zero)

    def finish(index, carry):
        at = pl.ds(pl.multiple_of(index * BLOCK, BLOCK), BLOCK)
        key = turn_back(dk_ref[at, :] * (1.0 / LOG2E), at)
        value = dv_ref[at, :].astype(jnp.bfloat16)
        out_ref[at, LANES : 2 * LANES] = key
        out_ref[at, 2 * LANES :] = value
        return (
            carry[0] + jnp.sum(key.astype(jnp.float32), axis=0, keepdims=True),
            carry[1] + jnp.sum(value.astype(jnp.float32), axis=0, keepdims=True),
        )

    key_bias, value_bias = lax.fori_loop(0, total // BLOCK, finish, (zero, zero))
    bias_ref[0] = jnp.concatenate([query_bias, key_bias, value_bias], axis=1)


def attend_back(qkv, mixed, mixed_grad, log_total, cosine, sine):
    total = qkv.shape[0]
    heads = mixed.shape[1] // LANES
    whole = lambda cols: pl.BlockSpec((total, cols), lambda h: (0, 0), pipeline_mode=pl.Buffered(1))
    wide = pl.BlockSpec((total, 3 * LANES), lambda h: (0, h))
    thin = pl.BlockSpec((total, LANES), lambda h: (0, h))
    return pl.pallas_call(
        back_kernel,
        grid=(heads,),
        in_specs=[
            wide,
            thin,
            thin,
            pl.BlockSpec((1, 1, total), lambda h: (h, 0, 0)),
            whole(LANES),
            whole(LANES),
        ],
        out_specs=[wide, pl.BlockSpec((1, 1, 3 * LANES), lambda h: (h, 0, 0))],
        out_shape=[
            jax.ShapeDtypeStruct((total, heads * 3 * LANES), jnp.bfloat16),
            jax.ShapeDtypeStruct((heads, 1, 3 * LANES), jnp.float32),
        ],
        scratch_shapes=[
            pltpu.VMEM((LANES, total), jnp.bfloat16),
            pltpu.VMEM((total, LANES), jnp.float32),
            pltpu.VMEM((total, LANES), jnp.float32),
        ],
        compiler_params=pltpu.CompilerParams(vmem_limit_bytes=40 * 2**20),
        cost_estimate=pl.CostEstimate(
            flops=2 * heads * total * total * LANES * 5,
            bytes_accessed=2 * total * heads * LANES * 8,
            transcendentals=heads * total * total,
        ),
    )(qkv, mixed, mixed_grad, log_total, cosine, sine)


def normalize(values, gain, shift):
    center = values - jnp.mean(values, axis=-1, keepdims=True)
    spread = lax.rsqrt(jnp.mean(center * center, axis=-1, keepdims=True) + epsilon)
    unit = center * spread
    return (unit * gain + shift, unit, spread)


def normalize_back(grads, unit, spread, gain):
    scaled = grads * gain
    inner = (
        scaled
        - jnp.mean(scaled, axis=-1, keepdims=True)
        - unit * jnp.mean(scaled * unit, axis=-1, keepdims=True)
    )
    return inner * spread


def swap(values):
    return lax.ppermute(values, "c", [(0, 1), (1, 0)])


def travel(step, size):
    runs = size // 2
    pairs = []
    for core in range(2):
        for place in range(size):
            half, part = divmod(place, runs)
            pairs.append((core * size + place, half * size + runs * core + (part + step) % runs))
    return pairs


def bring(packs, place, size):
    runs = size // 2
    parts = [
        lax.ppermute(
            lax.dynamic_index_in_dim(packs, lax.rem(place + step, runs), 0, keepdims=False),
            ("c", "z"),
            travel(step, size),
        )
        for step in range(runs)
    ]
    return jnp.concatenate(parts, axis=0)


def take_back(rows, place, size):
    runs = size // 2
    count = rows.shape[0] // runs
    parts = jnp.stack(
        [
            lax.ppermute(
                rows[step * count : (step + 1) * count],
                ("c", "z"),
                [(target, source) for source, target in travel(step, size)],
            )
            for step in range(runs)
        ]
    )
    return jnp.stack(
        [
            lax.dynamic_index_in_dim(
                parts, lax.rem(index + size - place, runs), 0, keepdims=False
            )
            for index in range(runs)
        ]
    )


def pair_sum(partial):
    count = partial.shape[0] // 2
    return partial[:count] + swap(partial[count:].astype(jnp.bfloat16)).astype(jnp.float32)


def share(own):
    return jnp.concatenate([own, swap(own)], axis=0)


def gather_all(block):
    return lax.all_gather(block, ("z", "g"), axis=0, tiled=True)


def flat(blocks):
    return blocks.reshape(-1, blocks.shape[-1])


def scatter_all(total):
    return lax.psum_scatter(total, ("z", "g"), scatter_dimension=0, tiled=True)


def sum_all(values):
    for axis in ("c", "g", "z"):
        size, apart = lax.axis_size(axis), 1
        assert size & (size - 1) == 0
        while apart < size:
            values = values + lax.ppermute(values, axis, [(i, i ^ apart) for i in range(size)])
            apart *= 2
    return values


def dot(form, left, right):
    return jnp.einsum(form, left, right, preferred_element_type=jnp.float32)


def on_device(
    hidden,
    positions,
    segments,
    ln1_gain,
    ln1_bias,
    qkv_weight,
    qkv_bias,
    proj_weight,
    proj_bias,
    ln2_gain,
    ln2_bias,
    fc1_weight,
    fc1_bias,
    fc2_weight,
    fc2_bias,
    cotangent,
):
    wide = jnp.float32
    size = lax.axis_size("z")
    core = lax.axis_index("c")
    place = lax.axis_index("z")
    group = lax.axis_index("g")
    batches, rows, width = hidden.shape
    runs = size // 2
    assert batches == runs
    shard = qkv_weight.shape[0]
    local_cols = qkv_weight.shape[2]
    half_cols = local_cols // 2
    units = fc1_weight.shape[1]
    half_units = units // 2
    pairs = half_cols // HEAD_DIM
    heads = size * pairs
    first = core == 0

    first_part = jnp.concatenate(
        [
            qkv_weight.reshape(shard, 3, 2, half_cols).transpose(0, 2, 1, 3).reshape(
                shard, 2, 3 * half_cols
            ),
            proj_weight.T.reshape(shard, 2, half_cols),
        ],
        axis=2,
    )
    packed = jnp.concatenate(
        [
            first_part,
            fc1_weight.reshape(shard, 2, half_units),
            fc2_weight.T.reshape(shard, 2, half_units),
        ],
        axis=2,
    )
    keep = jnp.where(first, packed[:, 0], packed[:, 1])
    other = swap(jnp.where(first, packed[:, 1], packed[:, 0]))
    block = jnp.where(
        first, jnp.concatenate([keep, other], axis=0), jnp.concatenate([other, keep], axis=0)
    )
    attn_cols = 4 * half_cols
    small = jnp.concatenate(
        [
            ln1_gain,
            ln1_bias,
            proj_bias,
            ln2_gain,
            ln2_bias,
            fc2_bias,
            qkv_bias.reshape(-1),
            fc1_bias,
        ]
    )
    length = small.shape[0]
    lines = -(-length // attn_cols)
    small = jnp.pad(small, (0, lines * attn_cols - length)).reshape(lines, attn_cols)
    small_other = swap(small)
    extra = -(-(2 * lines) // 16) * 16 - 2 * lines
    sent = jnp.concatenate(
        [
            block[:, :attn_cols],
            jnp.where(first, small, small_other),
            jnp.where(first, small_other, small),
            jnp.zeros((extra, attn_cols), small.dtype),
        ],
        axis=0,
    )
    arrived = gather_all(sent).reshape(size, -1, sent.shape[0], attn_cols)
    attn_full = arrived[:, :, : 2 * shard].reshape(size, width, attn_cols)
    small_full = arrived[:, :, 2 * shard : 2 * shard + 2 * lines].reshape(
        size, -1, lines * attn_cols
    )[:, :, :length]
    fc1_full = gather_all(block[:, attn_cols : attn_cols + half_units]).reshape(
        size, width, half_units
    )
    fc2_full = gather_all(block[:, attn_cols + half_units :]).reshape(size, width, half_units)
    qkv_table, proj_table = pad_tables(half_cols)
    qkv_full = dot("zdc,ck->zdk", attn_full, qkv_table).astype(jnp.bfloat16)
    proj_full = (
        dot("zdc,ck->dzk", attn_full, proj_table).astype(jnp.bfloat16).reshape(width, -1)
    )
    vectors = (
        small_full[0, :, : 6 * shard].reshape(-1, 6, shard).transpose(1, 0, 2).reshape(6, width)
    ).astype(wide)
    gain_one, shift_one, proj_shift, gain_two, shift_two, fc2_shift = (
        vectors[index] for index in range(6)
    )
    tail = small_full[:, 0, 6 * shard :].astype(wide)
    qkv_shifts = tail[:, : 3 * local_cols].reshape(size, 3, 2, half_cols)
    qkv_shift = jnp.where(first, qkv_shifts[:, :, 0], qkv_shifts[:, :, 1])
    qkv_shift = qkv_shift.reshape(size, 3, pairs, 2, MID).transpose(0, 2, 1, 3, 4)
    qkv_shift = jnp.pad(qkv_shift, ((0, 0),) * 4 + ((0, FREE),)).reshape(heads, 1, 3 * LANES)
    fc1_shifts = tail[:, 3 * local_cols :].reshape(size, 2, half_units)
    fc1_shift = jnp.where(first, fc1_shifts[:, 0], fc1_shifts[:, 1])

    marks = jnp.concatenate([positions, segments[:, None, :]], axis=1)
    marks_other = swap(marks)
    own_pack = place // runs == core
    batch = lax.rem(place, runs)
    marks = lax.dynamic_index_in_dim(
        jnp.where(own_pack, marks, marks_other), batch, 0, keepdims=False
    ).reshape(3, size, rows)
    order = [
        runs * (core if side == 0 else 1 - core) + lax.rem(batch + runs - step, runs)
        for side in range(2)
        for step in range(runs)
    ]
    marks = jnp.concatenate(
        [lax.dynamic_index_in_dim(marks, index, 1, keepdims=False) for index in order], axis=1
    )
    cosine, sine = angle_tables(marks[:2])
    query_mark, key_mark = label_tables(marks[2])

    start_values = bring(hidden, place, size).astype(wide)
    normed, unit_one, spread_one = normalize(start_values, gain_one, shift_one)
    normed_full = share(normed.astype(jnp.bfloat16))
    normed_full, cotangent = lax.optimization_barrier((normed_full, cotangent))
    out_grad = bring(cotangent, place, size)
    qkv, mixed, log_total = attend(
        normed_full, qkv_full, qkv_shift, cosine, sine, query_mark, key_mark
    )
    middle = start_values + pair_sum(dot("pk,dk->pd", mixed, proj_full)) + proj_shift
    normed_two, unit_two, spread_two = normalize(middle, gain_two, shift_two)
    ffn_input = share(normed_two.astype(jnp.bfloat16))
    before = dot("pd,zdf->pzf", ffn_input, fc1_full) + fc1_shift
    sigma = jax.nn.sigmoid(1.702 * before)
    after = (before * sigma).astype(jnp.bfloat16)
    outcome = middle + pair_sum(dot("pzf,zdf->pd", after, fc2_full)) + fc2_shift
    output = take_back(outcome.astype(jnp.bfloat16), place, size)

    out_grad_wide = out_grad.astype(wide)
    out_grad_full = share(out_grad)
    fc2_grad = flat(dot("pd,pzf->zdf", out_grad_full, after).astype(jnp.bfloat16))
    fc2_grad, out_grad_full = lax.optimization_barrier((fc2_grad, out_grad_full))
    fc2_part = scatter_all(fc2_grad)
    after_grad = dot("pd,zdf->pzf", out_grad_full, fc2_full)
    before_grad = (after_grad * (sigma + 1.702 * before * sigma * (1.0 - sigma))).astype(
        jnp.bfloat16
    )
    fc1_grad = flat(dot("pd,pzf->zdf", ffn_input, before_grad).astype(jnp.bfloat16))
    fc1_bias_total = jnp.sum(before_grad.astype(wide), axis=0)
    normed_two_grad = pair_sum(dot("pzf,zdf->pd", before_grad, fc1_full))
    middle_grad = out_grad_wide + normalize_back(normed_two_grad, unit_two, spread_two, gain_two)
    branch_grad_full = share(middle_grad.astype(jnp.bfloat16))
    branch_grad_full, fc1_grad = lax.optimization_barrier((branch_grad_full, fc1_grad))
    fc1_part = scatter_all(fc1_grad)
    proj_grad = dot("pd,pk->dk", branch_grad_full, mixed).astype(jnp.bfloat16)
    mixed_grad = dot("pd,dk->pk", branch_grad_full, proj_full).astype(jnp.bfloat16)
    projected_grad, qkv_bias_total = attend_back(
        qkv, mixed, mixed_grad, log_total, cosine, sine
    )
    split_grad = projected_grad.reshape(projected_grad.shape[0], size, -1)
    qkv_grad = dot("pd,pzk->zdk", normed_full, split_grad).astype(jnp.bfloat16)
    attn_part = scatter_all(
        flat(
            (
                dot("zdk,ck->zdc", qkv_grad, qkv_table)
                + dot("dzk,ck->zdc", proj_grad.reshape(width, size, -1), proj_table)
            ).astype(jnp.bfloat16)
        )
    )
    normed_grad = pair_sum(dot("pzk,zdk->pd", split_grad, qkv_full))
    hidden_grad = middle_grad + normalize_back(normed_grad, unit_one, spread_one, gain_one)
    input_grad = take_back(hidden_grad.astype(jnp.bfloat16), place, size)

    qkv_bias_total = qkv_bias_total.reshape(size, pairs, 3, 2, HALF)[..., :MID]
    qkv_bias_total = qkv_bias_total.transpose(0, 2, 1, 3, 4).reshape(size, 3 * half_cols)

    def halves(values):
        zero = jnp.zeros_like(values)
        return jnp.where(first, jnp.stack([values, zero], 1), jnp.stack([zero, values], 1))

    small_sums = sum_all(
        jnp.concatenate(
            [
                jnp.concatenate(
                    [
                        jnp.sum(normed_grad * unit_one, axis=0),
                        jnp.sum(normed_grad, axis=0),
                        jnp.sum(middle_grad, axis=0),
                        jnp.sum(normed_two_grad * unit_two, axis=0),
                        jnp.sum(normed_two_grad, axis=0),
                        jnp.sum(out_grad_wide, axis=0),
                    ]
                ),
                halves(qkv_bias_total).reshape(-1),
                halves(fc1_bias_total).reshape(-1),
            ]
        )
    )
    start = 6 * width
    vector_sums = lax.dynamic_slice_in_dim(
        small_sums[:start].reshape(6, width), (2 * group + core) * shard, shard, 1
    )
    middle_at = start + size * 3 * local_cols
    qkv_bias_sum = lax.dynamic_index_in_dim(
        small_sums[start:middle_at].reshape(size, 2, 3, half_cols), place, 0, keepdims=False
    )
    qkv_bias_sum = qkv_bias_sum.transpose(1, 0, 2).reshape(3, local_cols)
    fc1_bias_sum = lax.dynamic_index_in_dim(
        small_sums[middle_at:].reshape(size, units), place, 0, keepdims=False
    )

    def own_rows(part):
        mine = jnp.where(first, part[:shard], part[shard:])
        theirs = swap(jnp.where(first, part[shard:], part[:shard]))
        return jnp.where(first, jnp.stack([mine, theirs]), jnp.stack([theirs, mine])).astype(wide)

    fc2_sum = own_rows(fc2_part).transpose(0, 2, 1).reshape(units, shard)
    fc1_sum = own_rows(fc1_part).transpose(1, 0, 2).reshape(shard, units)
    attn_sum = own_rows(attn_part)
    qkv_sum = (
        attn_sum[:, :, : 3 * half_cols]
        .reshape(2, shard, 3, half_cols)
        .transpose(1, 2, 0, 3)
        .reshape(shard, 3, local_cols)
    )
    proj_sum = attn_sum[:, :, 3 * half_cols :].transpose(0, 2, 1).reshape(local_cols, shard)
    return (
        output,
        input_grad,
        vector_sums[0],
        vector_sums[1],
        qkv_sum,
        qkv_bias_sum,
        proj_sum,
        vector_sums[2],
        vector_sums[3],
        vector_sums[4],
        fc1_sum,
        fc1_bias_sum,
        fc2_sum,
        vector_sums[5],
    )


def solution(mesh):
    fsdp, tensor = mesh.shape["fsdp"], mesh.shape["tensor"]
    cut = Mesh(mesh.devices.reshape(fsdp // 2, 2, tensor), ("g", "c", "z"))
    f = ("g", "c")
    in_specs = (
        P(f, "z", None),
        P(f, None, None),
        P(f, None),
        P(f),
        P(f),
        P(f, None, "z"),
        P(None, "z"),
        P("z", f),
        P(f),
        P(f),
        P(f),
        P(f, "z"),
        P("z"),
        P("z", f),
        P(f),
        P(f, "z", None),
    )
    out_specs = (
        P(f, "z", None),
        P(f, "z", None),
        P(f),
        P(f),
        P(f, None, "z"),
        P(None, "z"),
        P("z", f),
        P(f),
        P(f),
        P(f),
        P(f, "z"),
        P("z"),
        P("z", f),
        P(f),
    )
    return jax.shard_map(
        on_device, mesh=cut, in_specs=in_specs, out_specs=out_specs, check_vma=False
    )
```

```python
import jax
import jax.numpy as jnp
import numpy as np
from jax import lax
from jax.experimental import pallas as pl
from jax.experimental.pallas import tpu as pltpu
from jax.sharding import Mesh, PartitionSpec as P


HEAD_DIM = 80

epsilon = 1e-06


LANES = 128
HALF = LANES // 2
MID = HEAD_DIM // 2
FREE = HALF - MID
FAR = -1.0e9
LOG2E = 1.4426950408889634
SCALE = HEAD_DIM ** (-0.5)
BLOCK = 256


def angle_tables(place):
    quarter = HEAD_DIM // 4
    freqs = 10000.0 ** (-(4.0 * jnp.arange(quarter, dtype=jnp.float32)) / HEAD_DIM)
    row_angles = place[0].astype(jnp.float32)[:, None] * freqs[None, :]
    col_angles = place[1].astype(jnp.float32)[:, None] * freqs[None, :]
    half = jnp.concatenate([row_angles, col_angles], axis=1)
    cosine = jnp.pad(jnp.cos(half), ((0, 0), (0, FREE)))
    sine = jnp.pad(jnp.sin(half), ((0, 0), (0, FREE)))
    return (
        jnp.concatenate([cosine, cosine], axis=1),
        jnp.concatenate([-sine, sine], axis=1),
    )


def label_tables(labels):
    lane = jnp.arange(LANES)[None, :] - MID
    free = (lane >= 0) & (lane < FREE)
    same = lane == labels[:, None]
    return (
        jnp.where(free & same, 1.0, 0.0).astype(jnp.bfloat16),
        jnp.where(free & ~same, FAR, 0.0).astype(jnp.bfloat16),
    )


def lane_of(index):
    return index if index < MID else index - MID + HALF


def pad_tables(cols):
    heads = cols // HEAD_DIM
    first = np.zeros((4 * cols, heads * 3 * LANES), np.float32)
    second = np.zeros((4 * cols, heads * LANES), np.float32)
    for head in range(heads):
        for index in range(HEAD_DIM):
            for kind in range(3):
                source = kind * cols + head * HEAD_DIM + index
                first[source, (head * 3 + kind) * LANES + lane_of(index)] = 1.0
            source = 3 * cols + head * HEAD_DIM + index
            second[source, head * LANES + lane_of(index)] = 1.0
    return jnp.asarray(first, jnp.bfloat16), jnp.asarray(second, jnp.bfloat16)


def product(left, right, dims):
    return lax.dot_general(left, right, (dims, ((), ())), preferred_element_type=jnp.float32)


def attend_kernel(
    x_ref, w_ref, b_ref, cos_ref, sin_ref, qa_ref, ka_ref, qkv_ref, o_ref, total_ref, vt_ref
):
    total = x_ref.shape[0]
    weight = w_ref[0]
    shift = b_ref[0]
    ones = jnp.where(lax.broadcasted_iota(jnp.int32, (BLOCK, LANES), 1) == LANES - 1, 1.0, 0.0)

    def project(index, carry):
        at = pl.ds(pl.multiple_of(index * BLOCK, BLOCK), BLOCK)
        made = product(x_ref[at, :], weight, ((1,), (0,))) + shift
        cosine, sine = cos_ref[at, :], sin_ref[at, :]
        query, key = made[:, :LANES], made[:, LANES : 2 * LANES]
        value = made[:, 2 * LANES :] + ones
        query = query * cosine + pltpu.roll(query, HALF, 1) * sine
        key = key * cosine + pltpu.roll(key, HALF, 1) * sine
        qkv_ref[at, :LANES] = (query * (SCALE * LOG2E)).astype(jnp.bfloat16) + qa_ref[at, :]
        qkv_ref[at, LANES : 2 * LANES] = key.astype(jnp.bfloat16) + ka_ref[at, :]
        qkv_ref[at, 2 * LANES :] = value.astype(jnp.bfloat16)
        vt_ref[:, at] = value.T.astype(jnp.bfloat16)
        return carry

    lax.fori_loop(0, total // BLOCK, project, 0)

    def mix(index, carry):
        at = pl.ds(pl.multiple_of(index * BLOCK, BLOCK), BLOCK)
        scores = product(qkv_ref[:, LANES : 2 * LANES], qkv_ref[at, :LANES], ((1,), (1,)))
        largest = jnp.max(scores, axis=0, keepdims=True)
        probs = jnp.exp2(scores - largest).astype(jnp.bfloat16)
        mixed = product(vt_ref[...], probs, ((1,), (0,)))
        amount = mixed[LANES - 1 :, :]
        o_ref[at, :] = (mixed * (1.0 / amount)).T.astype(jnp.bfloat16)
        total_ref[0, :, at] = largest + jnp.log2(amount)
        return carry

    lax.fori_loop(0, total // BLOCK, mix, 0)


def attend(normed, weight, shift, cosine, sine, query_mark, key_mark):
    total, width = normed.shape
    pairs = weight.shape[2] // (3 * LANES)
    heads = weight.shape[0] * pairs
    whole = lambda cols: pl.BlockSpec((total, cols), lambda h: (0, 0), pipeline_mode=pl.Buffered(1))
    return pl.pallas_call(
        attend_kernel,
        grid=(heads,),
        in_specs=[
            whole(width),
            pl.BlockSpec((1, width, 3 * LANES), lambda h: (h // pairs, 0, h % pairs)),
            pl.BlockSpec((1, 1, 3 * LANES), lambda h: (h, 0, 0)),
            whole(LANES),
            whole(LANES),
            whole(LANES),
            whole(LANES),
        ],
        out_specs=[
            pl.BlockSpec((total, 3 * LANES), lambda h: (0, h)),
            pl.BlockSpec((total, LANES), lambda h: (0, h)),
            pl.BlockSpec((1, 1, total), lambda h: (h, 0, 0)),
        ],
        out_shape=[
            jax.ShapeDtypeStruct((total, heads * 3 * LANES), jnp.bfloat16),
            jax.ShapeDtypeStruct((total, heads * LANES), jnp.bfloat16),
            jax.ShapeDtypeStruct((heads, 1, total), jnp.float32),
        ],
        scratch_shapes=[pltpu.VMEM((LANES, total), jnp.bfloat16)],
        compiler_params=pltpu.CompilerParams(vmem_limit_bytes=40 * 2**20),
        cost_estimate=pl.CostEstimate(
            flops=2 * heads * total * LANES * (3 * width + 4 * total),
            bytes_accessed=8 * total * heads * LANES + 2 * total * width,
            transcendentals=heads * total * total,
        ),
    )(normed, weight, shift, cosine, sine, query_mark, key_mark)


def back_kernel(
    qkv_ref, o_ref, grad_ref, total_ref, cos_ref, sin_ref, out_ref, bias_ref, kt_ref, dk_ref, dv_ref
):
    total = qkv_ref.shape[0]
    dk_ref[...] = jnp.zeros_like(dk_ref)
    dv_ref[...] = jnp.zeros_like(dv_ref)
    kt_ref[...] = qkv_ref[:, LANES : 2 * LANES].T

    def turn_back(grads, at):
        return (grads * cos_ref[at, :] + pltpu.roll(grads * sin_ref[at, :], HALF, 1)).astype(
            jnp.bfloat16
        )

    def step(index, carry):
        at = pl.ds(pl.multiple_of(index * BLOCK, BLOCK), BLOCK)
        query = qkv_ref[at, :LANES]
        grad = grad_ref[at, :]
        inner = grad.astype(jnp.float32) * o_ref[at, :].astype(jnp.float32)
        row = jnp.sum(inner.T, axis=0, keepdims=True)
        scores = product(qkv_ref[:, LANES : 2 * LANES], query, ((1,), (1,)))
        probs = jnp.exp2(scores - total_ref[0, :, at])
        weight_grad = product(qkv_ref[:, 2 * LANES :], grad, ((1,), (1,)))
        score_grad = (probs * (weight_grad - row)).astype(jnp.bfloat16)
        dv_ref[...] += product(probs.astype(jnp.bfloat16), grad, ((1,), (0,)))
        dk_ref[...] += product(score_grad, query, ((1,), (0,)))
        turned = product(kt_ref[...], score_grad, ((1,), (0,))).T * SCALE
        made = turn_back(turned, at)
        out_ref[at, :LANES] = made
        return carry + jnp.sum(made.astype(jnp.float32), axis=0, keepdims=True)

    zero = jnp.zeros((1, LANES), jnp.float32)
    query_bias = lax.fori_loop(0, total // BLOCK, step, zero)

    def finish(index, carry):
        at = pl.ds(pl.multiple_of(index * BLOCK, BLOCK), BLOCK)
        key = turn_back(dk_ref[at, :] * (1.0 / LOG2E), at)
        value = dv_ref[at, :].astype(jnp.bfloat16)
        out_ref[at, LANES : 2 * LANES] = key
        out_ref[at, 2 * LANES :] = value
        return (
            carry[0] + jnp.sum(key.astype(jnp.float32), axis=0, keepdims=True),
            carry[1] + jnp.sum(value.astype(jnp.float32), axis=0, keepdims=True),
        )

    key_bias, value_bias = lax.fori_loop(0, total // BLOCK, finish, (zero, zero))
    bias_ref[0] = jnp.concatenate([query_bias, key_bias, value_bias], axis=1)


def attend_back(qkv, mixed, mixed_grad, log_total, cosine, sine):
    total = qkv.shape[0]
    heads = mixed.shape[1] // LANES
    whole = lambda cols: pl.BlockSpec((total, cols), lambda h: (0, 0), pipeline_mode=pl.Buffered(1))
    wide = pl.BlockSpec((total, 3 * LANES), lambda h: (0, h))
    thin = pl.BlockSpec((total, LANES), lambda h: (0, h))
    return pl.pallas_call(
        back_kernel,
        grid=(heads,),
        in_specs=[
            wide,
            thin,
            thin,
            pl.BlockSpec((1, 1, total), lambda h: (h, 0, 0)),
            whole(LANES),
            whole(LANES),
        ],
        out_specs=[wide, pl.BlockSpec((1, 1, 3 * LANES), lambda h: (h, 0, 0))],
        out_shape=[
            jax.ShapeDtypeStruct((total, heads * 3 * LANES), jnp.bfloat16),
            jax.ShapeDtypeStruct((heads, 1, 3 * LANES), jnp.float32),
        ],
        scratch_shapes=[
            pltpu.VMEM((LANES, total), jnp.bfloat16),
            pltpu.VMEM((total, LANES), jnp.float32),
            pltpu.VMEM((total, LANES), jnp.float32),
        ],
        compiler_params=pltpu.CompilerParams(vmem_limit_bytes=40 * 2**20),
        cost_estimate=pl.CostEstimate(
            flops=2 * heads * total * total * LANES * 5,
            bytes_accessed=2 * total * heads * LANES * 8,
            transcendentals=heads * total * total,
        ),
    )(qkv, mixed, mixed_grad, log_total, cosine, sine)


def normalize(values, gain, shift):
    center = values - jnp.mean(values, axis=-1, keepdims=True)
    spread = lax.rsqrt(jnp.mean(center * center, axis=-1, keepdims=True) + epsilon)
    unit = center * spread
    return (unit * gain + shift, unit, spread)


def normalize_back(grads, unit, spread, gain):
    scaled = grads * gain
    inner = (
        scaled
        - jnp.mean(scaled, axis=-1, keepdims=True)
        - unit * jnp.mean(scaled * unit, axis=-1, keepdims=True)
    )
    return inner * spread


def swap(values):
    return lax.ppermute(values, "c", [(0, 1), (1, 0)])


def travel(step, size):
    runs = size // 2
    pairs = []
    for core in range(2):
        for place in range(size):
            half, part = divmod(place, runs)
            pairs.append((core * size + place, half * size + runs * core + (part + step) % runs))
    return pairs


def bring(packs, place, size):
    runs = size // 2
    parts = [
        lax.ppermute(
            lax.dynamic_index_in_dim(packs, lax.rem(place + step, runs), 0, keepdims=False),
            ("c", "z"),
            travel(step, size),
        )
        for step in range(runs)
    ]
    return jnp.concatenate(parts, axis=0)


def take_back(rows, place, size):
    runs = size // 2
    count = rows.shape[0] // runs
    parts = jnp.stack(
        [
            lax.ppermute(
                rows[step * count : (step + 1) * count],
                ("c", "z"),
                [(target, source) for source, target in travel(step, size)],
            )
            for step in range(runs)
        ]
    )
    return jnp.stack(
        [
            lax.dynamic_index_in_dim(
                parts, lax.rem(index + size - place, runs), 0, keepdims=False
            )
            for index in range(runs)
        ]
    )


def pair_sum(partial):
    count = partial.shape[0] // 2
    return partial[:count] + swap(partial[count:].astype(jnp.bfloat16)).astype(jnp.float32)


def share(own):
    return jnp.concatenate([own, swap(own)], axis=0)


def gather_all(block):
    return lax.all_gather(block, ("z", "g"), axis=0, tiled=True)


def flat(gathered, size):
    rows, cols = gathered.shape
    return gathered.reshape(size, rows // size, cols).transpose(1, 0, 2).reshape(rows // size, -1)


def scatter_rows(total):
    return lax.psum_scatter(total, "g", scatter_dimension=0, tiled=True)


def scatter_cols(part, place, size):
    cols = part.shape[1] // size

    def piece(index):
        return lax.dynamic_slice_in_dim(part, lax.rem(index, size) * cols, cols, 1)

    result = piece(place).astype(jnp.float32)
    for step in range(1, size):
        pairs = [(source, (source + step) % size) for source in range(size)]
        result = result + lax.ppermute(piece(place + step), "z", pairs).astype(jnp.float32)
    return result


def sum_all(values):
    for axis in ("c", "g", "z"):
        size, apart = lax.axis_size(axis), 1
        assert size & (size - 1) == 0
        while apart < size:
            values = values + lax.ppermute(values, axis, [(i, i ^ apart) for i in range(size)])
            apart *= 2
    return values


def dot(form, left, right):
    return jnp.einsum(form, left, right, preferred_element_type=jnp.float32)


def on_device(
    hidden,
    positions,
    segments,
    ln1_gain,
    ln1_bias,
    qkv_weight,
    qkv_bias,
    proj_weight,
    proj_bias,
    ln2_gain,
    ln2_bias,
    fc1_weight,
    fc1_bias,
    fc2_weight,
    fc2_bias,
    cotangent,
):
    wide = jnp.float32
    size = lax.axis_size("z")
    core = lax.axis_index("c")
    place = lax.axis_index("z")
    group = lax.axis_index("g")
    batches, rows, width = hidden.shape
    runs = size // 2
    assert batches == runs
    shard = qkv_weight.shape[0]
    local_cols = qkv_weight.shape[2]
    half_cols = local_cols // 2
    units = fc1_weight.shape[1]
    half_units = units // 2
    pairs = half_cols // HEAD_DIM
    heads = size * pairs
    first = core == 0

    first_part = jnp.concatenate(
        [
            qkv_weight.reshape(shard, 3, 2, half_cols).transpose(0, 2, 1, 3).reshape(
                shard, 2, 3 * half_cols
            ),
            proj_weight.T.reshape(shard, 2, half_cols),
        ],
        axis=2,
    )
    packed = jnp.concatenate(
        [
            first_part,
            fc1_weight.reshape(shard, 2, half_units),
            fc2_weight.T.reshape(shard, 2, half_units),
        ],
        axis=2,
    )
    keep = jnp.where(first, packed[:, 0], packed[:, 1])
    other = swap(jnp.where(first, packed[:, 1], packed[:, 0]))
    block = jnp.where(
        first, jnp.concatenate([keep, other], axis=0), jnp.concatenate([other, keep], axis=0)
    )
    attn_cols = 4 * half_cols
    small = jnp.concatenate(
        [
            ln1_gain,
            ln1_bias,
            proj_bias,
            ln2_gain,
            ln2_bias,
            fc2_bias,
            qkv_bias.reshape(-1),
            fc1_bias,
        ]
    )
    length = small.shape[0]
    lines = -(-length // attn_cols)
    small = jnp.pad(small, (0, lines * attn_cols - length)).reshape(lines, attn_cols)
    small_other = swap(small)
    extra = -(-(2 * lines) // 16) * 16 - 2 * lines
    sent = jnp.concatenate(
        [
            block[:, :attn_cols],
            jnp.where(first, small, small_other),
            jnp.where(first, small_other, small),
            jnp.zeros((extra, attn_cols), small.dtype),
        ],
        axis=0,
    )
    arrived = gather_all(sent).reshape(size, -1, sent.shape[0], attn_cols)
    attn_full = arrived[:, :, : 2 * shard].reshape(size, width, attn_cols)
    small_full = arrived[:, :, 2 * shard : 2 * shard + 2 * lines].reshape(
        size, -1, lines * attn_cols
    )[:, :, :length]
    fc1_full = flat(gather_all(block[:, attn_cols : attn_cols + half_units]), size)
    fc2_full = flat(gather_all(block[:, attn_cols + half_units :]), size)
    qkv_table, proj_table = pad_tables(half_cols)
    qkv_blocks = dot("zdc,ck->zdk", attn_full, qkv_table).astype(jnp.bfloat16)
    qkv_full = qkv_blocks.transpose(1, 0, 2).reshape(width, -1)
    proj_full = (
        dot("zdc,ck->dzk", attn_full, proj_table).astype(jnp.bfloat16).reshape(width, -1)
    )
    vectors = (
        small_full[0, :, : 6 * shard].reshape(-1, 6, shard).transpose(1, 0, 2).reshape(6, width)
    ).astype(wide)
    gain_one, shift_one, proj_shift, gain_two, shift_two, fc2_shift = (
        vectors[index] for index in range(6)
    )
    tail = small_full[:, 0, 6 * shard :].astype(wide)
    qkv_shifts = tail[:, : 3 * local_cols].reshape(size, 3, 2, half_cols)
    qkv_shift = jnp.where(first, qkv_shifts[:, :, 0], qkv_shifts[:, :, 1])
    qkv_shift = qkv_shift.reshape(size, 3, pairs, 2, MID).transpose(0, 2, 1, 3, 4)
    qkv_shift = jnp.pad(qkv_shift, ((0, 0),) * 4 + ((0, FREE),)).reshape(heads, 1, 3 * LANES)
    fc1_shifts = tail[:, 3 * local_cols :].reshape(size, 2, half_units)
    fc1_shift = jnp.where(first, fc1_shifts[:, 0], fc1_shifts[:, 1]).reshape(-1)

    marks = jnp.concatenate([positions, segments[:, None, :]], axis=1)
    marks_other = swap(marks)
    own_pack = place // runs == core
    batch = lax.rem(place, runs)
    marks = lax.dynamic_index_in_dim(
        jnp.where(own_pack, marks, marks_other), batch, 0, keepdims=False
    ).reshape(3, size, rows)
    order = [
        runs * (core if side == 0 else 1 - core) + lax.rem(batch + runs - step, runs)
        for side in range(2)
        for step in range(runs)
    ]
    marks = jnp.concatenate(
        [lax.dynamic_index_in_dim(marks, index, 1, keepdims=False) for index in order], axis=1
    )
    cosine, sine = angle_tables(marks[:2])
    query_mark, key_mark = label_tables(marks[2])

    start_values = bring(hidden, place, size).astype(wide)
    normed, unit_one, spread_one = normalize(start_values, gain_one, shift_one)
    normed_full = share(normed.astype(jnp.bfloat16))
    normed_full, cotangent = lax.optimization_barrier((normed_full, cotangent))
    out_grad = bring(cotangent, place, size)
    out_grad_full = share(out_grad)
    qkv, mixed, log_total = attend(
        normed_full, qkv_blocks, qkv_shift, cosine, sine, query_mark, key_mark
    )
    middle = start_values + pair_sum(dot("pk,dk->pd", mixed, proj_full)) + proj_shift
    normed_two, unit_two, spread_two = normalize(middle, gain_two, shift_two)
    ffn_input = share(normed_two.astype(jnp.bfloat16))
    before = dot("pd,df->pf", ffn_input, fc1_full) + fc1_shift
    sigma = jax.nn.sigmoid(1.702 * before)
    after = (before * sigma).astype(jnp.bfloat16)
    outcome = middle + pair_sum(dot("pf,df->pd", after, fc2_full)) + fc2_shift
    output = take_back(outcome.astype(jnp.bfloat16), place, size)

    out_grad_wide = out_grad.astype(wide)
    fc2_grad = dot("pd,pf->df", out_grad_full, after).astype(jnp.bfloat16)
    fc2_grad, out_grad_full = lax.optimization_barrier((fc2_grad, out_grad_full))
    fc2_rows = scatter_rows(fc2_grad)
    after_grad = dot("pd,df->pf", out_grad_full, fc2_full)
    before_grad = (after_grad * (sigma + 1.702 * before * sigma * (1.0 - sigma))).astype(
        jnp.bfloat16
    )
    fc1_grad = dot("pd,pf->df", ffn_input, before_grad).astype(jnp.bfloat16)
    fc1_bias_total = jnp.sum(before_grad.astype(wide), axis=0)
    normed_two_grad = pair_sum(dot("pf,df->pd", before_grad, fc1_full))
    middle_grad = out_grad_wide + normalize_back(normed_two_grad, unit_two, spread_two, gain_two)
    branch_grad_full = share(middle_grad.astype(jnp.bfloat16))
    branch_grad_full, fc1_grad = lax.optimization_barrier((branch_grad_full, fc1_grad))
    fc1_rows = scatter_rows(fc1_grad)
    proj_grad = dot("pd,pk->dk", branch_grad_full, mixed).astype(jnp.bfloat16)
    mixed_grad = dot("pd,dk->pk", branch_grad_full, proj_full).astype(jnp.bfloat16)
    fc2_part = scatter_cols(fc2_rows, place, size)
    projected_grad, qkv_bias_total = attend_back(qkv, mixed, mixed_grad, log_total, cosine, sine)
    qkv_grad = dot("pd,pk->dk", normed_full, projected_grad).astype(jnp.bfloat16)
    lanes = pairs * LANES
    attn_rows = scatter_rows(
        jnp.concatenate(
            [
                (
                    dot("dk,ck->dc", qkv_grad[:, 3 * lanes * n : 3 * lanes * (n + 1)], qkv_table)
                    + dot("dk,ck->dc", proj_grad[:, lanes * n : lanes * (n + 1)], proj_table)
                ).astype(jnp.bfloat16)
                for n in range(size)
            ],
            axis=1,
        )
    )
    fc1_part = scatter_cols(fc1_rows, place, size)
    normed_partial = dot("pk,dk->pd", projected_grad, qkv_full)
    normed_grad = pair_sum(normed_partial)
    attn_part = scatter_cols(attn_rows, place, size)
    hidden_grad = middle_grad + normalize_back(normed_grad, unit_one, spread_one, gain_one)
    input_grad = take_back(hidden_grad.astype(jnp.bfloat16), place, size)

    qkv_bias_total = qkv_bias_total.reshape(size, pairs, 3, 2, HALF)[..., :MID]
    qkv_bias_total = qkv_bias_total.transpose(0, 2, 1, 3, 4).reshape(size, 3 * half_cols)

    def halves(values):
        zero = jnp.zeros_like(values)
        return jnp.where(first, jnp.stack([values, zero], 1), jnp.stack([zero, values], 1))

    small_sums = sum_all(
        jnp.concatenate(
            [
                jnp.concatenate(
                    [
                        jnp.sum(normed_grad * unit_one, axis=0),
                        jnp.sum(normed_grad, axis=0),
                        jnp.sum(middle_grad, axis=0),
                        jnp.sum(normed_two_grad * unit_two, axis=0),
                        jnp.sum(normed_two_grad, axis=0),
                        jnp.sum(out_grad_wide, axis=0),
                    ]
                ),
                halves(qkv_bias_total).reshape(-1),
                halves(fc1_bias_total.reshape(size, half_units)).reshape(-1),
            ]
        )
    )
    start = 6 * width
    vector_sums = lax.dynamic_slice_in_dim(
        small_sums[:start].reshape(6, width), (2 * group + core) * shard, shard, 1
    )
    middle_at = start + size * 3 * local_cols
    qkv_bias_sum = lax.dynamic_index_in_dim(
        small_sums[start:middle_at].reshape(size, 2, 3, half_cols), place, 0, keepdims=False
    )
    qkv_bias_sum = qkv_bias_sum.transpose(1, 0, 2).reshape(3, local_cols)
    fc1_bias_sum = lax.dynamic_index_in_dim(
        small_sums[middle_at:].reshape(size, units), place, 0, keepdims=False
    )

    def own_rows(part):
        mine = jnp.where(first, part[:shard], part[shard:])
        theirs = jnp.where(first, part[shard:], part[:shard]).astype(jnp.bfloat16)
        theirs = swap(theirs).astype(wide)
        return jnp.where(first, jnp.stack([mine, theirs]), jnp.stack([theirs, mine]))

    fc2_sum = own_rows(fc2_part).transpose(0, 2, 1).reshape(units, shard)
    fc1_sum = own_rows(fc1_part).transpose(1, 0, 2).reshape(shard, units)
    attn_sum = own_rows(attn_part)
    qkv_sum = (
        attn_sum[:, :, : 3 * half_cols]
        .reshape(2, shard, 3, half_cols)
        .transpose(1, 2, 0, 3)
        .reshape(shard, 3, local_cols)
    )
    proj_sum = attn_sum[:, :, 3 * half_cols :].transpose(0, 2, 1).reshape(local_cols, shard)
    return (
        output,
        input_grad,
        vector_sums[0],
        vector_sums[1],
        qkv_sum,
        qkv_bias_sum,
        proj_sum,
        vector_sums[2],
        vector_sums[3],
        vector_sums[4],
        fc1_sum,
        fc1_bias_sum,
        fc2_sum,
        vector_sums[5],
    )


def solution(mesh):
    fsdp, tensor = mesh.shape["fsdp"], mesh.shape["tensor"]
    cut = Mesh(mesh.devices.reshape(fsdp // 2, 2, tensor), ("g", "c", "z"))
    f = ("g", "c")
    in_specs = (
        P(f, "z", None),
        P(f, None, None),
        P(f, None),
        P(f),
        P(f),
        P(f, None, "z"),
        P(None, "z"),
        P("z", f),
        P(f),
        P(f),
        P(f),
        P(f, "z"),
        P("z"),
        P("z", f),
        P(f),
        P(f, "z", None),
    )
    out_specs = (
        P(f, "z", None),
        P(f, "z", None),
        P(f),
        P(f),
        P(f, None, "z"),
        P(None, "z"),
        P("z", f),
        P(f),
        P(f),
        P(f),
        P(f, "z"),
        P("z"),
        P("z", f),
        P(f),
    )

    return jax.shard_map(
        on_device, mesh=cut, in_specs=in_specs, out_specs=out_specs, check_vma=False
    )
```

```python
import jax
import jax.numpy as jnp
import numpy as np
from jax import lax
from jax.experimental import pallas as pl
from jax.experimental.pallas import tpu as pltpu
from jax.sharding import Mesh, PartitionSpec as P


HEAD_DIM = 80

epsilon = 1e-06


LANES = 128
HALF = LANES // 2
MID = HEAD_DIM // 2
FREE = HALF - MID
FAR = -1.0e9
LOG2E = 1.4426950408889634
SCALE = HEAD_DIM ** (-0.5)
BLOCK = 256


def angle_tables(place):
    quarter = HEAD_DIM // 4
    freqs = 10000.0 ** (-(4.0 * jnp.arange(quarter, dtype=jnp.float32)) / HEAD_DIM)
    row_angles = place[0].astype(jnp.float32)[:, None] * freqs[None, :]
    col_angles = place[1].astype(jnp.float32)[:, None] * freqs[None, :]
    half = jnp.concatenate([row_angles, col_angles], axis=1)
    cosine = jnp.pad(jnp.cos(half), ((0, 0), (0, FREE)))
    sine = jnp.pad(jnp.sin(half), ((0, 0), (0, FREE)))
    return (
        jnp.concatenate([cosine, cosine], axis=1),
        jnp.concatenate([-sine, sine], axis=1),
    )


def label_tables(labels):
    lane = jnp.arange(LANES)[None, :] - MID
    free = (lane >= 0) & (lane < FREE)
    same = lane == labels[:, None]
    return (
        jnp.where(free & same, 1.0, 0.0).astype(jnp.bfloat16),
        jnp.where(free & ~same, FAR, 0.0).astype(jnp.bfloat16),
    )


def lane_of(index):
    return index if index < MID else index - MID + HALF


def pad_tables(cols):
    heads = cols // HEAD_DIM
    first = np.zeros((4 * cols, heads * 3 * LANES), np.float32)
    second = np.zeros((4 * cols, heads * LANES), np.float32)
    for head in range(heads):
        for index in range(HEAD_DIM):
            for kind in range(3):
                source = kind * cols + head * HEAD_DIM + index
                first[source, (head * 3 + kind) * LANES + lane_of(index)] = 1.0
            source = 3 * cols + head * HEAD_DIM + index
            second[source, head * LANES + lane_of(index)] = 1.0
    return jnp.asarray(first, jnp.bfloat16), jnp.asarray(second, jnp.bfloat16)


def product(left, right, dims):
    return lax.dot_general(left, right, (dims, ((), ())), preferred_element_type=jnp.float32)


def attend_kernel(
    x_ref, w_ref, b_ref, cos_ref, sin_ref, qa_ref, ka_ref, qkv_ref, o_ref, total_ref, vt_ref
):
    total = x_ref.shape[0]
    weight = w_ref[0]
    shift = b_ref[0]
    ones = jnp.where(lax.broadcasted_iota(jnp.int32, (BLOCK, LANES), 1) == LANES - 1, 1.0, 0.0)

    def project(index, carry):
        at = pl.ds(pl.multiple_of(index * BLOCK, BLOCK), BLOCK)
        made = product(x_ref[at, :], weight, ((1,), (0,))) + shift
        cosine, sine = cos_ref[at, :], sin_ref[at, :]
        query, key = made[:, :LANES], made[:, LANES : 2 * LANES]
        value = made[:, 2 * LANES :] + ones
        query = query * cosine + pltpu.roll(query, HALF, 1) * sine
        key = key * cosine + pltpu.roll(key, HALF, 1) * sine
        qkv_ref[at, :LANES] = (query * (SCALE * LOG2E)).astype(jnp.bfloat16) + qa_ref[at, :]
        qkv_ref[at, LANES : 2 * LANES] = key.astype(jnp.bfloat16) + ka_ref[at, :]
        qkv_ref[at, 2 * LANES :] = value.astype(jnp.bfloat16)
        vt_ref[:, at] = value.T.astype(jnp.bfloat16)
        return carry

    lax.fori_loop(0, total // BLOCK, project, 0, unroll=2)

    def mix(index, carry):
        at = pl.ds(pl.multiple_of(index * BLOCK, BLOCK), BLOCK)
        scores = product(qkv_ref[:, LANES : 2 * LANES], qkv_ref[at, :LANES], ((1,), (1,)))
        largest = jnp.max(scores, axis=0, keepdims=True)
        probs = jnp.exp2(scores - largest).astype(jnp.bfloat16)
        mixed = product(vt_ref[...], probs, ((1,), (0,)))
        amount = mixed[LANES - 1 :, :]
        o_ref[at, :] = (mixed * (1.0 / amount)).T.astype(jnp.bfloat16)
        total_ref[0, :, at] = largest + jnp.log2(amount)
        return carry

    lax.fori_loop(0, total // BLOCK, mix, 0, unroll=3)


def attend(normed, weight, shift, cosine, sine, query_mark, key_mark):
    total, width = normed.shape
    pairs = weight.shape[2] // (3 * LANES)
    heads = weight.shape[0] * pairs
    whole = lambda cols: pl.BlockSpec((total, cols), lambda h: (0, 0), pipeline_mode=pl.Buffered(1))
    return pl.pallas_call(
        attend_kernel,
        grid=(heads,),
        in_specs=[
            whole(width),
            pl.BlockSpec((1, width, 3 * LANES), lambda h: (h // pairs, 0, h % pairs)),
            pl.BlockSpec((1, 1, 3 * LANES), lambda h: (h, 0, 0)),
            whole(LANES),
            whole(LANES),
            whole(LANES),
            whole(LANES),
        ],
        out_specs=[
            pl.BlockSpec((total, 3 * LANES), lambda h: (0, h)),
            pl.BlockSpec((total, LANES), lambda h: (0, h)),
            pl.BlockSpec((1, 1, total), lambda h: (h, 0, 0)),
        ],
        out_shape=[
            jax.ShapeDtypeStruct((total, heads * 3 * LANES), jnp.bfloat16),
            jax.ShapeDtypeStruct((total, heads * LANES), jnp.bfloat16),
            jax.ShapeDtypeStruct((heads, 1, total), jnp.float32),
        ],
        scratch_shapes=[pltpu.VMEM((LANES, total), jnp.bfloat16)],
        compiler_params=pltpu.CompilerParams(vmem_limit_bytes=40 * 2**20),
        cost_estimate=pl.CostEstimate(
            flops=2 * heads * total * LANES * (3 * width + 4 * total),
            bytes_accessed=8 * total * heads * LANES + 2 * total * width,
            transcendentals=heads * total * total,
        ),
    )(normed, weight, shift, cosine, sine, query_mark, key_mark)


def back_kernel(
    qkv_ref, o_ref, grad_ref, total_ref, cos_ref, sin_ref, out_ref, bias_ref, kt_ref, dk_ref, dv_ref
):
    total = qkv_ref.shape[0]
    dk_ref[...] = jnp.zeros_like(dk_ref)
    dv_ref[...] = jnp.zeros_like(dv_ref)
    kt_ref[...] = qkv_ref[:, LANES : 2 * LANES].T

    def turn_back(grads, at):
        return (grads * cos_ref[at, :] + pltpu.roll(grads * sin_ref[at, :], HALF, 1)).astype(
            jnp.bfloat16
        )

    def step(index, carry):
        at = pl.ds(pl.multiple_of(index * BLOCK, BLOCK), BLOCK)
        query = qkv_ref[at, :LANES]
        grad = grad_ref[at, :]
        inner = grad.astype(jnp.float32) * o_ref[at, :].astype(jnp.float32)
        row = jnp.sum(inner.T, axis=0, keepdims=True)
        scores = product(qkv_ref[:, LANES : 2 * LANES], query, ((1,), (1,)))
        probs = jnp.exp2(scores - total_ref[0, :, at])
        weight_grad = product(qkv_ref[:, 2 * LANES :], grad, ((1,), (1,)))
        score_grad = (probs * (weight_grad - row)).astype(jnp.bfloat16)
        dv_ref[...] += product(probs.astype(jnp.bfloat16), grad, ((1,), (0,)))
        dk_ref[...] += product(score_grad, query, ((1,), (0,)))
        turned = product(kt_ref[...], score_grad, ((1,), (0,))).T * SCALE
        made = turn_back(turned, at)
        out_ref[at, :LANES] = made
        return carry + jnp.sum(made.astype(jnp.float32), axis=0, keepdims=True)

    zero = jnp.zeros((1, LANES), jnp.float32)
    query_bias = lax.fori_loop(0, total // BLOCK, step, zero)

    def finish(index, carry):
        at = pl.ds(pl.multiple_of(index * BLOCK, BLOCK), BLOCK)
        key = turn_back(dk_ref[at, :] * (1.0 / LOG2E), at)
        value = dv_ref[at, :].astype(jnp.bfloat16)
        out_ref[at, LANES : 2 * LANES] = key
        out_ref[at, 2 * LANES :] = value
        return (
            carry[0] + jnp.sum(key.astype(jnp.float32), axis=0, keepdims=True),
            carry[1] + jnp.sum(value.astype(jnp.float32), axis=0, keepdims=True),
        )

    key_bias, value_bias = lax.fori_loop(0, total // BLOCK, finish, (zero, zero))
    bias_ref[0] = jnp.concatenate([query_bias, key_bias, value_bias], axis=1)


def attend_back(qkv, mixed, mixed_grad, log_total, cosine, sine):
    total = qkv.shape[0]
    heads = mixed.shape[1] // LANES
    whole = lambda cols: pl.BlockSpec((total, cols), lambda h: (0, 0), pipeline_mode=pl.Buffered(1))
    wide = pl.BlockSpec((total, 3 * LANES), lambda h: (0, h))
    thin = pl.BlockSpec((total, LANES), lambda h: (0, h))
    return pl.pallas_call(
        back_kernel,
        grid=(heads,),
        in_specs=[
            wide,
            thin,
            thin,
            pl.BlockSpec((1, 1, total), lambda h: (h, 0, 0)),
            whole(LANES),
            whole(LANES),
        ],
        out_specs=[wide, pl.BlockSpec((1, 1, 3 * LANES), lambda h: (h, 0, 0))],
        out_shape=[
            jax.ShapeDtypeStruct((total, heads * 3 * LANES), jnp.bfloat16),
            jax.ShapeDtypeStruct((heads, 1, 3 * LANES), jnp.float32),
        ],
        scratch_shapes=[
            pltpu.VMEM((LANES, total), jnp.bfloat16),
            pltpu.VMEM((total, LANES), jnp.float32),
            pltpu.VMEM((total, LANES), jnp.float32),
        ],
        compiler_params=pltpu.CompilerParams(vmem_limit_bytes=40 * 2**20),
        cost_estimate=pl.CostEstimate(
            flops=2 * heads * total * total * LANES * 5,
            bytes_accessed=2 * total * heads * LANES * 8,
            transcendentals=heads * total * total,
        ),
    )(qkv, mixed, mixed_grad, log_total, cosine, sine)


def normalize(values, gain, shift):
    center = values - jnp.mean(values, axis=-1, keepdims=True)
    spread = lax.rsqrt(jnp.mean(center * center, axis=-1, keepdims=True) + epsilon)
    unit = center * spread
    return (unit * gain + shift, unit, spread)


def normalize_back(grads, unit, spread, gain):
    scaled = grads * gain
    inner = (
        scaled
        - jnp.mean(scaled, axis=-1, keepdims=True)
        - unit * jnp.mean(scaled * unit, axis=-1, keepdims=True)
    )
    return inner * spread


def swap(values):
    return lax.ppermute(values, "c", [(0, 1), (1, 0)])


def travel(step, size):
    runs = size // 2
    pairs = []
    for core in range(2):
        for place in range(size):
            half, part = divmod(place, runs)
            pairs.append((core * size + place, half * size + runs * core + (part + step) % runs))
    return pairs


def bring(packs, place, size):
    runs = size // 2
    parts = [
        lax.ppermute(
            lax.dynamic_index_in_dim(packs, lax.rem(place + step, runs), 0, keepdims=False),
            ("c", "z"),
            travel(step, size),
        )
        for step in range(runs)
    ]
    return jnp.concatenate(parts, axis=0)


def take_back(rows, place, size):
    runs = size // 2
    count = rows.shape[0] // runs
    parts = jnp.stack(
        [
            lax.ppermute(
                rows[step * count : (step + 1) * count],
                ("c", "z"),
                [(target, source) for source, target in travel(step, size)],
            )
            for step in range(runs)
        ]
    )
    return jnp.stack(
        [
            lax.dynamic_index_in_dim(
                parts, lax.rem(index + size - place, runs), 0, keepdims=False
            )
            for index in range(runs)
        ]
    )


def pair_sum(partial):
    count = partial.shape[0] // 2
    return partial[:count] + swap(partial[count:].astype(jnp.bfloat16)).astype(jnp.float32)


def share(own):
    return jnp.concatenate([own, swap(own)], axis=0)


def gather_all(block):
    return lax.all_gather(block, ("z", "g"), axis=0, tiled=True)


def flat(gathered, size):
    rows, cols = gathered.shape
    return gathered.reshape(size, rows // size, cols).transpose(1, 0, 2).reshape(rows // size, -1)


def scatter_rows(total):
    return lax.psum_scatter(total, "g", scatter_dimension=0, tiled=True)


def scatter_cols(part, place, size):
    cols = part.shape[1] // size

    def piece(index):
        return lax.dynamic_slice_in_dim(part, lax.rem(index, size) * cols, cols, 1)

    result = piece(place).astype(jnp.float32)
    for step in range(1, size):
        pairs = [(source, (source + step) % size) for source in range(size)]
        result = result + lax.ppermute(piece(place + step), "z", pairs).astype(jnp.float32)
    return result


def sum_all(values):
    for axis in ("c", "g", "z"):
        size, apart = lax.axis_size(axis), 1
        assert size & (size - 1) == 0
        while apart < size:
            moved = lax.ppermute(values, axis, [(i, i ^ apart) for i in range(size)])
            values = values + moved
            apart *= 2
    return values


def dot(form, left, right):
    return jnp.einsum(form, left, right, preferred_element_type=jnp.float32)


def on_device(
    hidden,
    positions,
    segments,
    ln1_gain,
    ln1_bias,
    qkv_weight,
    qkv_bias,
    proj_weight,
    proj_bias,
    ln2_gain,
    ln2_bias,
    fc1_weight,
    fc1_bias,
    fc2_weight,
    fc2_bias,
    cotangent,
):
    wide = jnp.float32
    size = lax.axis_size("z")
    core = lax.axis_index("c")
    place = lax.axis_index("z")
    group = lax.axis_index("g")
    batches, rows, width = hidden.shape
    runs = size // 2
    assert batches == runs
    shard = qkv_weight.shape[0]
    local_cols = qkv_weight.shape[2]
    half_cols = local_cols // 2
    units = fc1_weight.shape[1]
    half_units = units // 2
    pairs = half_cols // HEAD_DIM
    heads = size * pairs
    first = core == 0

    first_part = jnp.concatenate(
        [
            qkv_weight.reshape(shard, 3, 2, half_cols).transpose(0, 2, 1, 3).reshape(
                shard, 2, 3 * half_cols
            ),
            proj_weight.T.reshape(shard, 2, half_cols),
        ],
        axis=2,
    )
    packed = jnp.concatenate(
        [
            first_part,
            fc1_weight.reshape(shard, 2, half_units),
            fc2_weight.T.reshape(shard, 2, half_units),
        ],
        axis=2,
    )
    keep = jnp.where(first, packed[:, 0], packed[:, 1])
    other = swap(jnp.where(first, packed[:, 1], packed[:, 0]))
    block = jnp.where(
        first, jnp.concatenate([keep, other], axis=0), jnp.concatenate([other, keep], axis=0)
    )
    attn_cols = 4 * half_cols
    small = jnp.concatenate(
        [
            ln1_gain,
            ln1_bias,
            proj_bias,
            ln2_gain,
            ln2_bias,
            fc2_bias,
            qkv_bias.reshape(-1),
            fc1_bias,
        ]
    )
    length = small.shape[0]
    lines = -(-length // attn_cols)
    small = jnp.pad(small, (0, lines * attn_cols - length)).reshape(lines, attn_cols)
    small_other = swap(small)
    extra = -(-(2 * lines) // 16) * 16 - 2 * lines
    sent = jnp.concatenate(
        [
            block[:, :attn_cols],
            jnp.where(first, small, small_other),
            jnp.where(first, small_other, small),
            jnp.zeros((extra, attn_cols), small.dtype),
        ],
        axis=0,
    )
    arrived = gather_all(sent).reshape(size, -1, sent.shape[0], attn_cols)
    attn_full = arrived[:, :, : 2 * shard].reshape(size, width, attn_cols)
    small_full = arrived[:, :, 2 * shard : 2 * shard + 2 * lines].reshape(
        size, -1, lines * attn_cols
    )[:, :, :length]
    fc1_full = flat(gather_all(block[:, attn_cols : attn_cols + half_units]), size)
    fc2_full = gather_all(block[:, attn_cols + half_units :])
    fc2_full = flat(fc2_full, size)
    qkv_table, proj_table = pad_tables(half_cols)
    qkv_blocks = dot("zdc,ck->zdk", attn_full, qkv_table).astype(jnp.bfloat16)
    qkv_full = qkv_blocks.transpose(1, 0, 2).reshape(width, -1)
    proj_full = (
        dot("zdc,ck->dzk", attn_full, proj_table).astype(jnp.bfloat16).reshape(width, -1)
    )
    vectors = (
        small_full[0, :, : 6 * shard].reshape(-1, 6, shard).transpose(1, 0, 2).reshape(6, width)
    ).astype(wide)
    gain_one, shift_one, proj_shift, gain_two, shift_two, fc2_shift = (
        vectors[index] for index in range(6)
    )
    tail = small_full[:, 0, 6 * shard :].astype(wide)
    qkv_shifts = tail[:, : 3 * local_cols].reshape(size, 3, 2, half_cols)
    qkv_shift = jnp.where(first, qkv_shifts[:, :, 0], qkv_shifts[:, :, 1])
    qkv_shift = qkv_shift.reshape(size, 3, pairs, 2, MID).transpose(0, 2, 1, 3, 4)
    qkv_shift = jnp.pad(qkv_shift, ((0, 0),) * 4 + ((0, FREE),)).reshape(heads, 1, 3 * LANES)
    fc1_shifts = tail[:, 3 * local_cols :].reshape(size, 2, half_units)
    fc1_shift = jnp.where(first, fc1_shifts[:, 0], fc1_shifts[:, 1]).reshape(-1)

    marks = jnp.concatenate([positions, segments[:, None, :]], axis=1)
    marks_other = swap(marks)
    own_pack = place // runs == core
    batch = lax.rem(place, runs)
    marks = lax.dynamic_index_in_dim(
        jnp.where(own_pack, marks, marks_other), batch, 0, keepdims=False
    ).reshape(3, size, rows)
    order = [
        runs * (core if side == 0 else 1 - core) + lax.rem(batch + runs - step, runs)
        for side in range(2)
        for step in range(runs)
    ]
    marks = jnp.concatenate(
        [lax.dynamic_index_in_dim(marks, index, 1, keepdims=False) for index in order], axis=1
    )
    cosine, sine = angle_tables(marks[:2])
    query_mark, key_mark = label_tables(marks[2])

    start_values = bring(hidden, place, size).astype(wide)
    normed, unit_one, spread_one = normalize(start_values, gain_one, shift_one)
    normed_full = share(normed.astype(jnp.bfloat16))
    normed_full, cotangent = lax.optimization_barrier((normed_full, cotangent))
    out_grad = bring(cotangent, place, size)
    out_grad_full = share(out_grad)
    qkv, mixed, log_total = attend(
        normed_full, qkv_blocks, qkv_shift, cosine, sine, query_mark, key_mark
    )
    middle = start_values + pair_sum(dot("pk,dk->pd", mixed, proj_full)) + proj_shift
    normed_two, unit_two, spread_two = normalize(middle, gain_two, shift_two)
    ffn_input = share(normed_two.astype(jnp.bfloat16))
    before = dot("pd,df->pf", ffn_input, fc1_full)
    before = before + fc1_shift
    sigma = jax.nn.sigmoid(1.702 * before)
    after = (before * sigma).astype(jnp.bfloat16)
    outcome = middle + pair_sum(dot("pf,df->pd", after, fc2_full)) + fc2_shift
    output = take_back(outcome.astype(jnp.bfloat16), place, size)

    out_grad_wide = out_grad.astype(wide)
    fc2_grad = dot("pd,pf->df", out_grad_full, after).astype(jnp.bfloat16)
    fc2_grad, out_grad_full = lax.optimization_barrier((fc2_grad, out_grad_full))
    fc2_rows = scatter_rows(fc2_grad)
    after_grad = dot("pd,df->pf", out_grad_full, fc2_full)
    before_grad = (after_grad * (sigma + 1.702 * before * sigma * (1.0 - sigma))).astype(
        jnp.bfloat16
    )
    fc1_grad = dot("pd,pf->df", ffn_input, before_grad).astype(jnp.bfloat16)
    fc1_bias_total = jnp.sum(before_grad.astype(wide), axis=0)
    normed_two_grad = pair_sum(dot("pf,df->pd", before_grad, fc1_full))
    middle_grad = out_grad_wide + normalize_back(normed_two_grad, unit_two, spread_two, gain_two)
    branch_grad_full = share(middle_grad.astype(jnp.bfloat16))
    branch_grad_full, fc1_grad = lax.optimization_barrier((branch_grad_full, fc1_grad))
    fc1_rows = scatter_rows(fc1_grad)
    proj_grad = dot("pd,pk->dk", branch_grad_full, mixed).astype(jnp.bfloat16)
    mixed_grad = dot("pd,dk->pk", branch_grad_full, proj_full).astype(jnp.bfloat16)
    fc2_part = scatter_cols(fc2_rows, place, size)
    projected_grad, qkv_bias_total = attend_back(qkv, mixed, mixed_grad, log_total, cosine, sine)
    qkv_grad = dot("pd,pk->dk", normed_full, projected_grad).astype(jnp.bfloat16)
    lanes = pairs * LANES
    attn_rows = scatter_rows(
        jnp.concatenate(
            [
                (
                    dot("dk,ck->dc", qkv_grad[:, 3 * lanes * n : 3 * lanes * (n + 1)], qkv_table)
                    + dot("dk,ck->dc", proj_grad[:, lanes * n : lanes * (n + 1)], proj_table)
                ).astype(jnp.bfloat16)
                for n in range(size)
            ],
            axis=1,
        )
    )
    fc1_part = scatter_cols(fc1_rows, place, size)
    normed_partial = dot("pk,dk->pd", projected_grad, qkv_full)
    normed_grad = pair_sum(normed_partial)
    attn_part = scatter_cols(attn_rows, place, size)
    hidden_grad = middle_grad + normalize_back(normed_grad, unit_one, spread_one, gain_one)
    input_grad = take_back(hidden_grad.astype(jnp.bfloat16), place, size)

    qkv_bias_total = qkv_bias_total.reshape(size, pairs, 3, 2, HALF)[..., :MID]
    qkv_bias_total = qkv_bias_total.transpose(0, 2, 1, 3, 4).reshape(size, 3 * half_cols)

    def halves(values):
        zero = jnp.zeros_like(values)
        return jnp.where(first, jnp.stack([values, zero], 1), jnp.stack([zero, values], 1))

    small_sums = sum_all(
        jnp.concatenate(
            [
                jnp.concatenate(
                    [
                        jnp.sum(normed_grad * unit_one, axis=0),
                        jnp.sum(normed_grad, axis=0),
                        jnp.sum(middle_grad, axis=0),
                        jnp.sum(normed_two_grad * unit_two, axis=0),
                        jnp.sum(normed_two_grad, axis=0),
                        jnp.sum(out_grad_wide, axis=0),
                    ]
                ),
                halves(qkv_bias_total).reshape(-1),
                halves(fc1_bias_total.reshape(size, half_units)).reshape(-1),
            ]
        )
    )
    start = 6 * width
    vector_sums = lax.dynamic_slice_in_dim(
        small_sums[:start].reshape(6, width), (2 * group + core) * shard, shard, 1
    )
    middle_at = start + size * 3 * local_cols
    qkv_bias_sum = lax.dynamic_index_in_dim(
        small_sums[start:middle_at].reshape(size, 2, 3, half_cols), place, 0, keepdims=False
    )
    qkv_bias_sum = qkv_bias_sum.transpose(1, 0, 2).reshape(3, local_cols)
    fc1_bias_sum = lax.dynamic_index_in_dim(
        small_sums[middle_at:].reshape(size, units), place, 0, keepdims=False
    )

    def own_rows(part):
        mine = jnp.where(first, part[:shard], part[shard:])
        theirs = jnp.where(first, part[shard:], part[:shard]).astype(jnp.bfloat16)
        theirs = swap(theirs).astype(wide)
        return jnp.where(first, jnp.stack([mine, theirs]), jnp.stack([theirs, mine]))

    fc2_sum = own_rows(fc2_part).transpose(0, 2, 1).reshape(units, shard)
    fc1_sum = own_rows(fc1_part).transpose(1, 0, 2).reshape(shard, units)
    attn_sum = own_rows(attn_part)
    qkv_sum = (
        attn_sum[:, :, : 3 * half_cols]
        .reshape(2, shard, 3, half_cols)
        .transpose(1, 2, 0, 3)
        .reshape(shard, 3, local_cols)
    )
    proj_sum = attn_sum[:, :, 3 * half_cols :].transpose(0, 2, 1).reshape(local_cols, shard)
    return (
        output,
        input_grad,
        vector_sums[0],
        vector_sums[1],
        qkv_sum,
        qkv_bias_sum,
        proj_sum,
        vector_sums[2],
        vector_sums[3],
        vector_sums[4],
        fc1_sum,
        fc1_bias_sum,
        fc2_sum,
        vector_sums[5],
    )


def solution(mesh):
    fsdp, tensor = mesh.shape["fsdp"], mesh.shape["tensor"]
    cut = Mesh(mesh.devices.reshape(fsdp // 2, 2, tensor), ("g", "c", "z"))
    f = ("g", "c")
    in_specs = (
        P(f, "z", None),
        P(f, None, None),
        P(f, None),
        P(f),
        P(f),
        P(f, None, "z"),
        P(None, "z"),
        P("z", f),
        P(f),
        P(f),
        P(f),
        P(f, "z"),
        P("z"),
        P("z", f),
        P(f),
        P(f, "z", None),
    )
    out_specs = (
        P(f, "z", None),
        P(f, "z", None),
        P(f),
        P(f),
        P(f, None, "z"),
        P(None, "z"),
        P("z", f),
        P(f),
        P(f),
        P(f),
        P(f, "z"),
        P("z"),
        P("z", f),
        P(f),
    )

    return jax.shard_map(
        on_device, mesh=cut, in_specs=in_specs, out_specs=out_specs, check_vma=False
    )
```
